16 devices in a mesh: fsdp: 2 (over z), ep: 8 (over y, x, core).
Axes of the slice: x: 2, y: 2, z: 2, core: 2. Of those that a mesh axis runs over, the one named last changes fastest.
Arguments:
- grad_out: bfloat16 [32768, 768], P(('fsdp', 'ep'))
- expert_idx: int32 [32768, 1], P(('fsdp', 'ep'))
- slot_pos: int32 [32768, 1], P(('fsdp', 'ep'))
- gates: float32 [32768, 1], P(('fsdp', 'ep'))
- x_disp: bfloat16 [8, 5120, 768], P('ep', 'fsdp')
- h_gate: bfloat16 [8, 5120, 3072], P('ep', 'fsdp')
- h_up: bfloat16 [8, 5120, 3072], P('ep', 'fsdp')
- y_disp: bfloat16 [8, 5120, 768], P('ep', 'fsdp')
- w_gate: bfloat16 [8, 768, 3072], P('ep', 'fsdp')
- w_down: bfloat16 [8, 3072, 768], P('ep', 'fsdp')
- w_up: bfloat16 [8, 768, 3072], P('ep', 'fsdp')
Outputs:
- output 1: bfloat16 [32768, 768], P(('fsdp', 'ep'))
- output 2: float32 [32768, 1], P(('fsdp', 'ep'))
- output 3: float32 [8, 768, 3072], P('ep', 'fsdp')
- output 4: float32 [8, 3072, 768], P('ep', 'fsdp')
- output 5: float32 [8, 768, 3072], P('ep', 'fsdp')
All inputs are finite; a program needn't handle non-finite values.
Results may differ from the reference program's by a relative error of at most 0.001.
Values are sent between devices in bfloat16 or wider.
A program may use at most 1 GiB of HBM per device.

```python
import jax
import jax.numpy as jnp
from jax import lax

D = 768
F = 3072
EXPERTS = 8
TOP = 1
TOK = 2048
NDEV = 16
CAP = 320


def route_draw(key):
    key_bias, key_noise, key_hot = jax.random.split(key, 3)
    expert_ids = jnp.arange(EXPERTS, dtype=jnp.int32)
    expert_bias = jax.random.randint(key_bias, (EXPERTS,), 0, 512, dtype=jnp.int32)
    noise_int = jax.random.randint(key_noise, (NDEV, TOK, EXPERTS), 0, 1024, dtype=jnp.int32)
    hot_expert = jax.random.randint(key_hot, (NDEV,), 0, EXPERTS, dtype=jnp.int32)
    forced = (jnp.arange(TOK, dtype=jnp.int32)[None, :, None] <= CAP) & (expert_ids[None, None, :] == hot_expert[:, None, None])
    score_int = (noise_int + expert_bias + jnp.where(forced, 4096, 0)) * EXPERTS + expert_ids
    expert_idx = lax.top_k(score_int, TOP)[1].astype(jnp.int32)

    def block_slots(block_idx):
        flat_ids = block_idx.reshape(-1)
        hit_mask = (flat_ids[:, None] == expert_ids[None, :]).astype(jnp.int32)
        slot_rank = jnp.sum((jnp.cumsum(hit_mask, axis=0) - hit_mask) * hit_mask, axis=1)
        return jnp.where(slot_rank < CAP, slot_rank, -1).reshape(TOK, TOP)

    slot_pos = lax.map(block_slots, expert_idx)
    return expert_idx.reshape(NDEV * TOK, TOP), slot_pos.reshape(NDEV * TOK, TOP).astype(jnp.int32)


def setup_inputs(seed: int = 0) -> dict:
    keys = jax.random.split(jax.random.key(seed), 11)
    expert_idx, slot_pos = route_draw(keys[0])
    rows_all = NDEV * CAP
    grad_out = jax.random.normal(keys[1], (NDEV * TOK, D), jnp.float32).astype(jnp.bfloat16)
    gates = jax.random.uniform(keys[2], (NDEV * TOK, TOP), jnp.float32, 0.2, 1.0)
    x_disp = jax.random.normal(keys[3], (EXPERTS, rows_all, D), jnp.float32).astype(jnp.bfloat16)
    h_gate = jax.random.normal(keys[4], (EXPERTS, rows_all, F), jnp.float32).astype(jnp.bfloat16)
    h_up = jax.random.normal(keys[5], (EXPERTS, rows_all, F), jnp.float32).astype(jnp.bfloat16)
    y_disp = (0.25 * jax.random.normal(keys[6], (EXPERTS, rows_all, D), jnp.float32)).astype(jnp.bfloat16)
    w_gate = (jax.random.normal(keys[7], (EXPERTS, D, F), jnp.float32) * D ** -0.5).astype(jnp.bfloat16)
    w_down = (jax.random.normal(keys[8], (EXPERTS, F, D), jnp.float32) * F ** -0.5).astype(jnp.bfloat16)
    w_up = (jax.random.normal(keys[9], (EXPERTS, D, F), jnp.float32) * D ** -0.5).astype(jnp.bfloat16)
    return {'grad_out': grad_out, 'expert_idx': expert_idx, 'slot_pos': slot_pos, 'gates': gates, 'x_disp': x_disp, 'h_gate': h_gate, 'h_up': h_up, 'y_disp': y_disp, 'w_gate': w_gate, 'w_down': w_down, 'w_up': w_up}


def expert_backward(operands):
    dy_rows, gate_rows, x_rows, pre_gate, pre_up, y_rows, w_gate, w_down, w_up = operands
    g_rows = (dy_rows.astype(jnp.float32) * gate_rows[:, None]).astype(jnp.bfloat16)
    gate_pre = pre_gate.astype(jnp.float32)
    up_pre = pre_up.astype(jnp.float32)
    sigmoid_gate = jax.nn.sigmoid(gate_pre)
    silu_gate = gate_pre * sigmoid_gate
    act_rows = (silu_gate * up_pre).astype(jnp.bfloat16)
    d_act = jnp.dot(g_rows, w_down.T, preferred_element_type=jnp.float32)
    dh_gate = (d_act * up_pre * sigmoid_gate * (1.0 + gate_pre * (1.0 - sigmoid_gate))).astype(jnp.bfloat16)
    dh_up = (d_act * silu_gate).astype(jnp.bfloat16)
    dx_rows = (jnp.dot(dh_gate, w_gate.T, preferred_element_type=jnp.float32) + jnp.dot(dh_up, w_up.T, preferred_element_type=jnp.float32)).astype(jnp.bfloat16)
    dgate_rows = jnp.sum(dy_rows.astype(jnp.float32) * y_rows.astype(jnp.float32), axis=1)
    dw_gate = jnp.dot(x_rows.T, dh_gate, preferred_element_type=jnp.float32)
    dw_down = jnp.dot(act_rows.T, g_rows, preferred_element_type=jnp.float32)
    dw_up = jnp.dot(x_rows.T, dh_up, preferred_element_type=jnp.float32)
    return dx_rows, dgate_rows, dw_gate, dw_down, dw_up


def reference(grad_out, expert_idx, slot_pos, gates, x_disp, h_gate, h_up, y_disp, w_gate, w_down, w_up):
    rows_all = NDEV * CAP
    choices = NDEV * TOK * TOP
    block_ids = jnp.arange(NDEV * TOK, dtype=jnp.int32)[:, None] // TOK
    dest_row = jnp.where(slot_pos >= 0, expert_idx * rows_all + block_ids * CAP + slot_pos, EXPERTS * rows_all).reshape(-1)
    src_choice = jnp.full((EXPERTS * rows_all,), choices, jnp.int32).at[dest_row].set(jnp.arange(choices, dtype=jnp.int32), mode='drop')
    dy_rows = jnp.take(grad_out, src_choice // TOP, axis=0, mode='fill', fill_value=0).reshape(EXPERTS, rows_all, D)
    gate_rows = jnp.take(gates.reshape(-1), src_choice, mode='fill', fill_value=0).reshape(EXPERTS, rows_all)
    dx_rows, dgate_rows, dw_gate, dw_down, dw_up = lax.map(expert_backward, (dy_rows, gate_rows, x_disp, h_gate, h_up, y_disp, w_gate, w_down, w_up))
    picked = jnp.take(dx_rows.reshape(EXPERTS * rows_all, D), dest_row, axis=0, mode='fill', fill_value=0).reshape(NDEV * TOK, TOP, D)
    grad_x = jnp.sum(picked.astype(jnp.float32), axis=1).astype(jnp.bfloat16)
    grad_gates = jnp.take(dgate_rows.reshape(-1), dest_row, mode='fill', fill_value=0).reshape(NDEV * TOK, TOP)
    return grad_x, grad_gates, dw_gate, dw_down, dw_up
```

```python
import jax
import jax.numpy as jnp
from jax import lax
from jax.sharding import PartitionSpec as P


F32 = jnp.float32
BF16 = jnp.bfloat16


def solution(mesh):
    ep_n = mesh.shape['ep']
    fs_n = mesh.shape['fsdp']
    tok_spec = P(('fsdp', 'ep'), None)
    row_spec = P('ep', 'fsdp', None)
    swap = [(i, fs_n - 1 - i) for i in range(fs_n)]

    def exchange(value):
        return lax.ppermute(value, 'fsdp', swap)

    def local_backward(grad_out, expert_idx, slot_pos, gates, x_disp, h_gate, h_up, y_disp, w_gate, w_down, w_up):
        tok_n, top_n = expert_idx.shape
        e_loc, rows_loc, width = x_disp.shape
        slot_cap = rows_loc // ep_n
        slots_n = e_loc * ep_n * slot_cap
        choices = tok_n * top_n
        z = lax.axis_index('fsdp')

        other_w_down = exchange(w_down)
        other_w_gate = exchange(w_gate)
        other_w_up = exchange(w_up)

        def whole(own, other):
            return jnp.where(z == 0, jnp.concatenate([own, other], axis=1), jnp.concatenate([other, own], axis=1))

        send_row = jnp.where(slot_pos >= 0, ((expert_idx % e_loc) * ep_n + expert_idx // e_loc) * slot_cap + slot_pos, slots_n).reshape(-1)
        src_choice = jnp.full((slots_n,), choices, jnp.int32).at[send_row].set(jnp.arange(choices, dtype=jnp.int32), mode='drop')
        send_dy = jnp.take(grad_out, src_choice // top_n, axis=0, mode='fill', fill_value=0).reshape(e_loc, ep_n, slot_cap, width)
        send_gate = jnp.take(gates.reshape(-1), src_choice, mode='fill', fill_value=0).reshape(e_loc, ep_n, slot_cap)
        dy_rows = lax.all_to_all(send_dy, 'ep', 1, 1, tiled=True).reshape(e_loc, rows_loc, width)
        gate_rows = lax.all_to_all(send_gate, 'ep', 1, 1, tiled=True).reshape(e_loc, rows_loc)

        g_rows = (dy_rows.astype(F32) * gate_rows[..., None]).astype(BF16)
        gate_pre = h_gate.astype(F32)
        up_pre = h_up.astype(F32)
        sigmoid_gate = jax.nn.sigmoid(gate_pre)
        silu_gate = gate_pre * sigmoid_gate
        act_rows = (silu_gate * up_pre).astype(BF16)

        def part(value, axis, index):
            half = value.shape[axis] // fs_n
            return lax.dynamic_slice_in_dim(value, index * half, half, axis)

        send = jnp.einsum('erf,erd->efd', part(act_rows, 2, 1 - z), g_rows, preferred_element_type=F32)
        recv_dw_down = exchange(send)

        full_w_down = whole(w_down, other_w_down)
        d_act = jnp.einsum('erd,efd->erf', g_rows, full_w_down, preferred_element_type=F32)
        dh_gate = (d_act * up_pre * sigmoid_gate * (1.0 + gate_pre * (1.0 - sigmoid_gate))).astype(BF16)
        dh_up = (d_act * silu_gate).astype(BF16)

        x_send = part(x_disp, 2, 1 - z)
        x_own = part(x_disp, 2, z)
        recv_dw_gate = exchange(jnp.einsum('erd,erf->edf', x_send, dh_gate, preferred_element_type=F32))
        recv_dw_up = exchange(jnp.einsum('erd,erf->edf', x_send, dh_up, preferred_element_type=F32))

        full_w_gate = whole(w_gate, other_w_gate)
        full_w_up = whole(w_up, other_w_up)
        dx_rows = (jnp.einsum('erf,edf->erd', dh_gate, full_w_gate, preferred_element_type=F32) + jnp.einsum('erf,edf->erd', dh_up, full_w_up, preferred_element_type=F32)).astype(BF16)
        dgate_rows = jnp.einsum('erd,erd->er', dy_rows, y_disp, preferred_element_type=F32)
        back_dx = lax.all_to_all(dx_rows.reshape(e_loc, ep_n, slot_cap, width), 'ep', 1, 1, tiled=True).reshape(slots_n, width)
        back_gate = lax.all_to_all(dgate_rows.reshape(e_loc, ep_n, slot_cap), 'ep', 1, 1, tiled=True).reshape(slots_n)
        picked = jnp.take(back_dx, send_row, axis=0, mode='fill', fill_value=0).reshape(tok_n, top_n, width)
        grad_x = jnp.sum(picked.astype(F32), axis=1).astype(BF16)
        grad_gates = jnp.take(back_gate, send_row, mode='fill', fill_value=0).reshape(tok_n, top_n)

        def combine(own, recv):
            return lax.optimization_barrier(own) + recv

        grad_w_down = combine(jnp.einsum('erf,erd->efd', part(act_rows, 2, z), g_rows, preferred_element_type=F32), recv_dw_down)
        grad_w_gate = combine(jnp.einsum('erd,erf->edf', x_own, dh_gate, preferred_element_type=F32), recv_dw_gate)
        grad_w_up = combine(jnp.einsum('erd,erf->edf', x_own, dh_up, preferred_element_type=F32), recv_dw_up)
        return grad_x, grad_gates, grad_w_gate, grad_w_down, grad_w_up

    return jax.shard_map(local_backward, mesh=mesh, in_specs=(tok_spec, tok_spec, tok_spec, tok_spec, row_spec, row_spec, row_spec, row_spec, row_spec, row_spec, row_spec), out_specs=(tok_spec, tok_spec, row_spec, row_spec, row_spec), check_vma=False)
```

```python
import jax
import jax.numpy as jnp
from jax import lax
from jax.experimental import pallas as pl
from jax.experimental.pallas import tpu as pltpu
from jax.sharding import PartitionSpec as P


F32 = jnp.float32
BF16 = jnp.bfloat16
VMEM_LIMIT = 67043328


def params(*kinds):
    return pltpu.CompilerParams(dimension_semantics=kinds, vmem_limit_bytes=VMEM_LIMIT)


def cost(flops, bytes_accessed):
    return pl.CostEstimate(flops=flops, bytes_accessed=bytes_accessed, transcendentals=0)


def hidden_grads(z, g_rows, w_own, w_other, h_gate, h_up, row_tile=512, col_tile=512):
    rows, width = g_rows.shape
    half = w_own.shape[0]
    tiles = half // col_tile
    row_steps = rows // row_tile

    def col(z_ref, h, j):
        return jnp.where(h == 0, z_ref[0], 1 - z_ref[0]) * tiles + j

    def kernel(z_ref, g_ref, own_ref, other_ref, h1_ref, h3_ref, d1_ref, d3_ref, a_ref):
        h, i = pl.program_id(0), pl.program_id(2)
        g = g_ref[pl.ds(pl.multiple_of(i * row_tile, row_tile), row_tile), :]
        w = jnp.where(h == 0, own_ref[...], other_ref[...])
        d_act = lax.dot_general(g, w, (((1,), (1,)), ((), ())), preferred_element_type=F32)
        h1 = h1_ref[...].astype(F32)
        h3 = h3_ref[...].astype(F32)
        sig = jax.nn.sigmoid(h1)
        silu = h1 * sig
        a_ref[...] = (silu * h3).astype(BF16)
        d1_ref[...] = (d_act * h3 * sig * (1.0 + h1 * (1.0 - sig))).astype(BF16)
        d3_ref[...] = (d_act * silu).astype(BF16)

    tile = pl.BlockSpec((row_tile, col_tile), lambda h, j, i, z_ref: (i, col(z_ref, h, j)))
    return pl.pallas_call(
        kernel,
        grid_spec=pltpu.PrefetchScalarGridSpec(
            num_scalar_prefetch=1,
            grid=(2, tiles, row_steps),
            in_specs=[
                pl.BlockSpec((rows, width), lambda h, j, i, z_ref: (0, 0)),
                pl.BlockSpec((col_tile, width), lambda h, j, i, z_ref: (jnp.where(h == 0, j, tiles - 1), 0)),
                pl.BlockSpec((col_tile, width), lambda h, j, i, z_ref: (jnp.where(h == 0, 0, j), 0)),
                tile, tile,
            ],
            out_specs=[tile] * 3,
        ),
        out_shape=[jax.ShapeDtypeStruct(h_gate.shape, BF16)] * 3,
        compiler_params=params('arbitrary', 'arbitrary', 'arbitrary'),
        cost_estimate=cost(2 * rows * width * 2 * half, 10 * rows * 2 * half),
    )(z, g_rows, w_own, w_other, h_gate, h_up)


def weight_grad_lhs(which, wide, rhs, halves, col_tile=512):
    rows, cols = wide.shape
    width = rhs.shape[1]
    tiles = cols // halves // col_tile

    def kernel(s_ref, l_ref, r_ref, o_ref):
        o_ref[...] = lax.dot_general(l_ref[...], r_ref[...], (((0,), (0,)), ((), ())), preferred_element_type=F32)

    return pl.pallas_call(
        kernel,
        grid_spec=pltpu.PrefetchScalarGridSpec(
            num_scalar_prefetch=1,
            grid=(tiles,),
            in_specs=[
                pl.BlockSpec((rows, col_tile), lambda j, s_ref: (0, s_ref[0] * tiles + j)),
                pl.BlockSpec((rows, width), lambda j, s_ref: (0, 0)),
            ],
            out_specs=pl.BlockSpec((col_tile, width), lambda j, s_ref: (j, 0)),
        ),
        out_shape=jax.ShapeDtypeStruct((tiles * col_tile, width), F32),
        compiler_params=params('arbitrary'),
        cost_estimate=cost(2 * rows * width * tiles * col_tile, rows * cols + 4 * width * cols),
    )(which, wide, rhs)


def weight_grad_rhs(which, x_rows, wide, halves, col_tile=512):
    rows, cols = wide.shape
    part = x_rows.shape[1] // halves

    def kernel(s_ref, l_ref, r_ref, o_ref):
        o_ref[...] = lax.dot_general(l_ref[...], r_ref[...], (((0,), (0,)), ((), ())), preferred_element_type=F32)

    return pl.pallas_call(
        kernel,
        grid_spec=pltpu.PrefetchScalarGridSpec(
            num_scalar_prefetch=1,
            grid=(cols // col_tile,),
            in_specs=[
                pl.BlockSpec((rows, part), lambda j, s_ref: (0, s_ref[0])),
                pl.BlockSpec((rows, col_tile), lambda j, s_ref: (0, j)),
            ],
            out_specs=pl.BlockSpec((part, col_tile), lambda j, s_ref: (0, j)),
        ),
        out_shape=jax.ShapeDtypeStruct((part, cols), F32),
        compiler_params=params('arbitrary'),
        cost_estimate=cost(2 * rows * part * cols, 2 * rows * cols + 4 * part * cols),
    )(which, x_rows, wide)


def row_grads(z, dh_gate, dh_up, gate_own, gate_other, up_own, up_other, row_tile=256):
    rows, cols = dh_gate.shape
    part = gate_own.shape[0]

    def kernel(z_ref, d1_ref, d3_ref, g0_ref, g1_ref, u0_ref, u1_ref, o_ref):
        h = pl.program_id(0)
        dims = (((1,), (1,)), ((), ()))

        def emit(w1_ref, w3_ref):
            acc = lax.dot_general(d1_ref[...], w1_ref[...], dims, preferred_element_type=F32)
            acc += lax.dot_general(d3_ref[...], w3_ref[...], dims, preferred_element_type=F32)
            o_ref[...] = acc.astype(BF16)

        pl.when(h == 0)(lambda: emit(g0_ref, u0_ref))
        pl.when(h == 1)(lambda: emit(g1_ref, u1_ref))

    tile = pl.BlockSpec((row_tile, cols), lambda h, i, z_ref: (i, 0))
    full = pl.BlockSpec((part, cols), lambda h, i, z_ref: (0, 0))
    return pl.pallas_call(
        kernel,
        grid_spec=pltpu.PrefetchScalarGridSpec(
            num_scalar_prefetch=1,
            grid=(2, rows // row_tile),
            in_specs=[tile, tile, full, full, full, full],
            out_specs=pl.BlockSpec((row_tile, part), lambda h, i, z_ref: (i, jnp.where(h == 0, z_ref[0], 1 - z_ref[0]))),
        ),
        out_shape=jax.ShapeDtypeStruct((rows, 2 * part), BF16),
        compiler_params=params('arbitrary', 'arbitrary'),
        cost_estimate=cost(8 * rows * cols * part, 8 * rows * cols),
    )(z, dh_gate, dh_up, gate_own, gate_other, up_own, up_other)


def add_rows(own, recv, first, tile):
    rows, width = recv.shape
    base = first // tile

    def kernel(own_ref, recv_ref, o_ref):
        o_ref[...] = own_ref[...] + recv_ref[...]

    return pl.pallas_call(
        kernel,
        grid=(rows // tile,),
        in_specs=[pl.BlockSpec((tile, width), lambda i: (base + i, 0)), pl.BlockSpec((tile, width), lambda i: (i, 0))],
        out_specs=pl.BlockSpec((tile, width), lambda i: (base + i, 0)),
        out_shape=jax.ShapeDtypeStruct(own.shape, own.dtype),
        input_output_aliases={0: 0},
        compiler_params=params('arbitrary'),
        cost_estimate=cost(rows * width, 12 * rows * width),
    )(own, recv)


def solution(mesh):
    ep_n = mesh.shape['ep']
    fs_n = mesh.shape['fsdp']
    tok_spec = P(('fsdp', 'ep'), None)
    row_spec = P('ep', 'fsdp', None)
    swap = [(i, fs_n - 1 - i) for i in range(fs_n)]

    def exchange(value):
        return lax.ppermute(value, 'fsdp', swap)

    def local_backward(grad_out, expert_idx, slot_pos, gates, x_disp, h_gate, h_up, y_disp, w_gate, w_down, w_up):
        tok_n, top_n = expert_idx.shape
        e_loc, rows_loc, width = x_disp.shape
        slot_cap = rows_loc // ep_n
        slots_n = e_loc * ep_n * slot_cap
        choices = tok_n * top_n
        x_rows, y_rows, h_gate, h_up, w_gate, w_down, w_up = (v[0] for v in (x_disp, y_disp, h_gate, h_up, w_gate, w_down, w_up))

        z = lax.axis_index('fsdp').reshape(1).astype(jnp.int32)
        other_w_down = exchange(w_down)
        other_w_gate = exchange(w_gate)
        other_w_up = exchange(w_up)

        send_row = jnp.where(slot_pos >= 0, ((expert_idx % e_loc) * ep_n + expert_idx // e_loc) * slot_cap + slot_pos, slots_n).reshape(-1)
        src_choice = jnp.full((slots_n,), choices, jnp.int32).at[send_row].set(jnp.arange(choices, dtype=jnp.int32), mode='drop')
        send_dy = jnp.take(grad_out, src_choice // top_n, axis=0, mode='fill', fill_value=0).reshape(e_loc, ep_n, slot_cap, width)
        send_gate = jnp.take(gates.reshape(-1), src_choice, mode='fill', fill_value=0).reshape(e_loc, ep_n, slot_cap)
        dy_rows = lax.all_to_all(send_dy, 'ep', 1, 1, tiled=True).reshape(rows_loc, width)
        gate_rows = lax.all_to_all(send_gate, 'ep', 1, 1, tiled=True).reshape(rows_loc)
        g_rows = (dy_rows.astype(F32) * gate_rows[:, None]).astype(BF16)

        dh_gate, dh_up, act = hidden_grads(z, g_rows, w_down, other_w_down, h_gate, h_up)
        send = weight_grad_lhs(1 - z, act, g_rows, fs_n)
        recv_down = exchange(send)
        send = weight_grad_rhs(1 - z, x_rows, dh_gate, fs_n)
        recv_gate = exchange(send)
        send = weight_grad_rhs(1 - z, x_rows, dh_up, fs_n)
        step = send.shape[0] // 16
        cuts = (0, 12 * step, 15 * step, 16 * step)
        recv_up = [exchange(send[lo:hi]) for lo, hi in zip(cuts, cuts[1:])]

        dx_rows = row_grads(z, dh_gate, dh_up, w_gate, other_w_gate, w_up, other_w_up)
        dgate_rows = jnp.einsum('rd,rd->r', dy_rows, y_rows, preferred_element_type=F32)
        back_dx = lax.all_to_all(dx_rows.reshape(e_loc, ep_n, slot_cap, width), 'ep', 1, 1, tiled=True).reshape(slots_n, width)
        back_gate = lax.all_to_all(dgate_rows.reshape(e_loc, ep_n, slot_cap), 'ep', 1, 1, tiled=True).reshape(slots_n)
        picked = jnp.take(back_dx, send_row, axis=0, mode='fill', fill_value=0).reshape(tok_n, top_n, width)
        grad_x = jnp.sum(picked.astype(F32), axis=1).astype(BF16)
        grad_gates = jnp.take(back_gate, send_row, mode='fill', fill_value=0).reshape(tok_n, top_n)

        grad_w_down = weight_grad_lhs(z, act, g_rows, fs_n)
        grad_w_gate = weight_grad_rhs(z, x_rows, dh_gate, fs_n)
        grad_w_up = weight_grad_rhs(z, x_rows, dh_up, fs_n)
        grad_w_down = add_rows(grad_w_down, recv_down, 0, 128)
        grad_w_gate = add_rows(grad_w_gate, recv_gate, 0, 2 * step)
        for n, recv in enumerate(recv_up):
            grad_w_up = add_rows(grad_w_up, recv, cuts[n], step)
        return grad_x, grad_gates, grad_w_gate[None], grad_w_down[None], grad_w_up[None]

    return jax.shard_map(local_backward, mesh=mesh, in_specs=(tok_spec, tok_spec, tok_spec, tok_spec, row_spec, row_spec, row_spec, row_spec, row_spec, row_spec, row_spec), out_specs=(tok_spec, tok_spec, row_spec, row_spec, row_spec), check_vma=False)
```

```python
import jax
import jax.numpy as jnp
from jax import lax
from jax.experimental import pallas as pl
from jax.experimental.pallas import tpu as pltpu
from jax.sharding import PartitionSpec as P


F32 = jnp.float32
BF16 = jnp.bfloat16
VMEM_LIMIT = 67043328


def params(*kinds):
    return pltpu.CompilerParams(dimension_semantics=kinds, vmem_limit_bytes=VMEM_LIMIT)


def cost(flops, bytes_accessed):
    return pl.CostEstimate(flops=flops, bytes_accessed=bytes_accessed, transcendentals=0)


def hidden_grads(z, g_rows, w_own, w_other, h_gate, h_up, row_tile=512, col_tile=512):
    rows, width = g_rows.shape
    half = w_own.shape[0]
    tiles = half // col_tile
    row_steps = rows // row_tile

    def col(z_ref, h, j):
        return jnp.where(h == 0, z_ref[0], 1 - z_ref[0]) * tiles + j

    def kernel(z_ref, g_ref, own_ref, other_ref, h1_ref, h3_ref, d1_ref, d3_ref):
        h, i = pl.program_id(0), pl.program_id(2)
        g = g_ref[pl.ds(pl.multiple_of(i * row_tile, row_tile), row_tile), :]
        w = jnp.where(h == 0, own_ref[...], other_ref[...])
        d_act = lax.dot_general(g, w, (((1,), (1,)), ((), ())), preferred_element_type=F32)
        h1 = h1_ref[...].astype(F32)
        h3 = h3_ref[...].astype(F32)
        sig = jax.nn.sigmoid(h1)
        silu = h1 * sig
        d1_ref[...] = (d_act * h3 * sig * (1.0 + h1 * (1.0 - sig))).astype(BF16)
        d3_ref[...] = (d_act * silu).astype(BF16)

    tile = pl.BlockSpec((row_tile, col_tile), lambda h, j, i, z_ref: (i, col(z_ref, h, j)))
    return pl.pallas_call(
        kernel,
        grid_spec=pltpu.PrefetchScalarGridSpec(
            num_scalar_prefetch=1,
            grid=(2, tiles, row_steps),
            in_specs=[
                pl.BlockSpec((rows, width), lambda h, j, i, z_ref: (0, 0)),
                pl.BlockSpec((col_tile, width), lambda h, j, i, z_ref: (jnp.where(h == 0, j, tiles - 1), 0)),
                pl.BlockSpec((col_tile, width), lambda h, j, i, z_ref: (jnp.where(h == 0, 0, j), 0)),
                tile, tile,
            ],
            out_specs=[tile] * 2,
        ),
        out_shape=[jax.ShapeDtypeStruct(h_gate.shape, BF16)] * 2,
        compiler_params=params('arbitrary', 'arbitrary', 'arbitrary'),
        cost_estimate=cost(2 * rows * width * 2 * half, 8 * rows * 2 * half),
    )(z, g_rows, w_own, w_other, h_gate, h_up)


def down_grad(which, h_gate, h_up, g_rows, halves, row_tile=512, col_tile=512):
    rows, cols = h_gate.shape
    width = g_rows.shape[1]
    tiles = cols // halves // col_tile

    def kernel(s_ref, h1_ref, h3_ref, g_ref, o_ref):
        i = pl.program_id(1)
        h1 = h1_ref[...].astype(F32)
        act = (h1 * jax.nn.sigmoid(h1) * h3_ref[...].astype(F32)).astype(BF16)
        g = g_ref[pl.ds(pl.multiple_of(i * row_tile, row_tile), row_tile), :]
        term = lax.dot_general(act, g, (((0,), (0,)), ((), ())), preferred_element_type=F32)

        @pl.when(i == 0)
        def _():
            o_ref[...] = term

        @pl.when(i > 0)
        def _():
            o_ref[...] += term

    tile = pl.BlockSpec((row_tile, col_tile), lambda j, i, s_ref: (i, s_ref[0] * tiles + j))
    return pl.pallas_call(
        kernel,
        grid_spec=pltpu.PrefetchScalarGridSpec(
            num_scalar_prefetch=1,
            grid=(tiles, rows // row_tile),
            in_specs=[tile, tile, pl.BlockSpec((rows, width), lambda j, i, s_ref: (0, 0))],
            out_specs=pl.BlockSpec((col_tile, width), lambda j, i, s_ref: (j, 0)),
        ),
        out_shape=jax.ShapeDtypeStruct((tiles * col_tile, width), F32),
        compiler_params=params('arbitrary', 'arbitrary'),
        cost_estimate=cost(2 * rows * width * tiles * col_tile, 4 * rows * cols),
    )(which, h_gate, h_up, g_rows)


def weight_grad_rhs(which, x_rows, wide, halves, col_tile=512):
    rows, cols = wide.shape
    part = x_rows.shape[1] // halves

    def kernel(s_ref, l_ref, r_ref, o_ref):
        o_ref[...] = lax.dot_general(l_ref[...], r_ref[...], (((0,), (0,)), ((), ())), preferred_element_type=F32)

    return pl.pallas_call(
        kernel,
        grid_spec=pltpu.PrefetchScalarGridSpec(
            num_scalar_prefetch=1,
            grid=(cols // col_tile,),
            in_specs=[
                pl.BlockSpec((rows, part), lambda j, s_ref: (0, s_ref[0])),
                pl.BlockSpec((rows, col_tile), lambda j, s_ref: (0, j)),
            ],
            out_specs=pl.BlockSpec((part, col_tile), lambda j, s_ref: (0, j)),
        ),
        out_shape=jax.ShapeDtypeStruct((part, cols), F32),
        compiler_params=params('arbitrary'),
        cost_estimate=cost(2 * rows * part * cols, 2 * rows * cols + 4 * part * cols),
    )(which, x_rows, wide)


def row_grads(z, dh_gate, dh_up, gate_own, gate_other, up_own, up_other, row_tile=256):
    rows, cols = dh_gate.shape
    part = gate_own.shape[0]

    def kernel(z_ref, d1_ref, d3_ref, g0_ref, g1_ref, u0_ref, u1_ref, o_ref):
        h = pl.program_id(0)
        dims = (((1,), (1,)), ((), ()))

        def emit(w1_ref, w3_ref):
            acc = lax.dot_general(d1_ref[...], w1_ref[...], dims, preferred_element_type=F32)
            acc += lax.dot_general(d3_ref[...], w3_ref[...], dims, preferred_element_type=F32)
            o_ref[...] = acc.astype(BF16)

        pl.when(h == 0)(lambda: emit(g0_ref, u0_ref))
        pl.when(h == 1)(lambda: emit(g1_ref, u1_ref))

    tile = pl.BlockSpec((row_tile, cols), lambda h, i, z_ref: (i, 0))
    full = pl.BlockSpec((part, cols), lambda h, i, z_ref: (0, 0))
    return pl.pallas_call(
        kernel,
        grid_spec=pltpu.PrefetchScalarGridSpec(
            num_scalar_prefetch=1,
            grid=(2, rows // row_tile),
            in_specs=[tile, tile, full, full, full, full],
            out_specs=pl.BlockSpec((row_tile, part), lambda h, i, z_ref: (i, jnp.where(h == 0, z_ref[0], 1 - z_ref[0]))),
        ),
        out_shape=jax.ShapeDtypeStruct((rows, 2 * part), BF16),
        compiler_params=params('arbitrary', 'arbitrary'),
        cost_estimate=cost(8 * rows * cols * part, 8 * rows * cols),
    )(z, dh_gate, dh_up, gate_own, gate_other, up_own, up_other)


def add_rows(own, recv, first, tile):
    rows, width = recv.shape
    base = first // tile

    def kernel(own_ref, recv_ref, o_ref):
        o_ref[...] = own_ref[...] + recv_ref[...]

    return pl.pallas_call(
        kernel,
        grid=(rows // tile,),
        in_specs=[pl.BlockSpec((tile, width), lambda i: (base + i, 0)), pl.BlockSpec((tile, width), lambda i: (i, 0))],
        out_specs=pl.BlockSpec((tile, width), lambda i: (base + i, 0)),
        out_shape=jax.ShapeDtypeStruct(own.shape, own.dtype),
        input_output_aliases={0: 0},
        compiler_params=params('arbitrary'),
        cost_estimate=cost(rows * width, 12 * rows * width),
    )(own, recv)


def solution(mesh):
    ep_n = mesh.shape['ep']
    fs_n = mesh.shape['fsdp']
    tok_spec = P(('fsdp', 'ep'), None)
    row_spec = P('ep', 'fsdp', None)
    swap = [(i, fs_n - 1 - i) for i in range(fs_n)]

    def exchange(value):
        return lax.ppermute(value, 'fsdp', swap)

    def local_backward(grad_out, expert_idx, slot_pos, gates, x_disp, h_gate, h_up, y_disp, w_gate, w_down, w_up):
        tok_n, top_n = expert_idx.shape
        e_loc, rows_loc, width = x_disp.shape
        slot_cap = rows_loc // ep_n
        slots_n = e_loc * ep_n * slot_cap
        choices = tok_n * top_n
        x_rows, y_rows, h_gate, h_up, w_gate, w_down, w_up = (v[0] for v in (x_disp, y_disp, h_gate, h_up, w_gate, w_down, w_up))

        z = lax.axis_index('fsdp').reshape(1).astype(jnp.int32)
        other_w_down = exchange(w_down)
        other_w_gate = exchange(w_gate)
        other_w_up = exchange(w_up)

        send_row = jnp.where(slot_pos >= 0, ((expert_idx % e_loc) * ep_n + expert_idx // e_loc) * slot_cap + slot_pos, slots_n).reshape(-1)
        src_choice = jnp.full((slots_n,), choices, jnp.int32).at[send_row].set(jnp.arange(choices, dtype=jnp.int32), mode='drop')
        send_dy = jnp.take(grad_out, src_choice // top_n, axis=0, mode='fill', fill_value=0).reshape(e_loc, ep_n, slot_cap, width)
        send_gate = jnp.take(gates.reshape(-1), src_choice, mode='fill', fill_value=0).reshape(e_loc, ep_n, slot_cap)
        dy_rows = lax.all_to_all(send_dy, 'ep', 1, 1, tiled=True).reshape(rows_loc, width)
        gate_rows = lax.all_to_all(send_gate, 'ep', 1, 1, tiled=True).reshape(rows_loc)
        g_rows = (dy_rows.astype(F32) * gate_rows[:, None]).astype(BF16)

        send = down_grad(1 - z, h_gate, h_up, g_rows, fs_n)
        recv_down = exchange(send)
        dh_gate, dh_up = hidden_grads(z, g_rows, w_down, other_w_down, h_gate, h_up)
        send = weight_grad_rhs(1 - z, x_rows, dh_gate, fs_n)
        recv_gate = exchange(send)
        send = weight_grad_rhs(1 - z, x_rows, dh_up, fs_n)
        step = send.shape[0] // 16
        cuts = (0, 12 * step, 15 * step, 15 * step + 2 * step // 3, 16 * step)
        tiles = (4 * step, 3 * step, step // 3, step // 3)
        recv_up = [exchange(send[lo:hi]) for lo, hi in zip(cuts, cuts[1:])]

        dx_rows = row_grads(z, dh_gate, dh_up, w_gate, other_w_gate, w_up, other_w_up)
        dgate_rows = jnp.einsum('rd,rd->r', dy_rows, y_rows, preferred_element_type=F32)
        back_dx = lax.all_to_all(dx_rows.reshape(e_loc, ep_n, slot_cap, width), 'ep', 1, 1, tiled=True).reshape(slots_n, width)
        back_gate = lax.all_to_all(dgate_rows.reshape(e_loc, ep_n, slot_cap), 'ep', 1, 1, tiled=True).reshape(slots_n)
        picked = jnp.take(back_dx, send_row, axis=0, mode='fill', fill_value=0).reshape(tok_n, top_n, width)
        grad_x = jnp.sum(picked.astype(F32), axis=1).astype(BF16)
        grad_gates = jnp.take(back_gate, send_row, mode='fill', fill_value=0).reshape(tok_n, top_n)

        grad_w_down = down_grad(z, h_gate, h_up, g_rows, fs_n)
        grad_w_gate = weight_grad_rhs(z, x_rows, dh_gate, fs_n)
        grad_w_up = weight_grad_rhs(z, x_rows, dh_up, fs_n)
        grad_w_down = add_rows(grad_w_down, recv_down, 0, 384)
        grad_w_gate = add_rows(grad_w_gate, recv_gate, 0, 4 * step)
        for n, recv in enumerate(recv_up):
            grad_w_up = add_rows(grad_w_up, recv, cuts[n], tiles[n])
        return grad_x, grad_gates, grad_w_gate[None], grad_w_down[None], grad_w_up[None]

    return jax.shard_map(local_backward, mesh=mesh, in_specs=(tok_spec, tok_spec, tok_spec, tok_spec, row_spec, row_spec, row_spec, row_spec, row_spec, row_spec, row_spec), out_specs=(tok_spec, tok_spec, row_spec, row_spec, row_spec), check_vma=False)
```

```python
import jax
import jax.numpy as jnp
from jax import lax
from jax.experimental import pallas as pl
from jax.experimental.pallas import tpu as pltpu
from jax.sharding import PartitionSpec as P


F32 = jnp.float32
BF16 = jnp.bfloat16
VMEM_LIMIT = 58 * 1024 * 1024


def params(*kinds):
    return pltpu.CompilerParams(dimension_semantics=kinds, vmem_limit_bytes=VMEM_LIMIT)


def cost(flops, bytes_accessed):
    return pl.CostEstimate(flops=flops, bytes_accessed=bytes_accessed, transcendentals=0)


def hidden_grads(z, g_rows, w_own, w_other, h_gate, h_up, row_tile=512, col_tile=512):
    rows, width = g_rows.shape
    half = w_own.shape[0]
    tiles = half // col_tile
    row_steps = rows // row_tile

    def col(z_ref, h, j):
        return jnp.where(h == 0, z_ref[0], 1 - z_ref[0]) * tiles + j

    def kernel(z_ref, g_ref, own_ref, other_ref, h1_ref, h3_ref, d1_ref, d3_ref):
        h, i = pl.program_id(0), pl.program_id(2)
        g = g_ref[pl.ds(pl.multiple_of(i * row_tile, row_tile), row_tile), :]
        w = jnp.where(h == 0, own_ref[...], other_ref[...])
        d_act = lax.dot_general(g, w, (((1,), (1,)), ((), ())), preferred_element_type=F32)
        h1 = h1_ref[...].astype(F32)
        h3 = h3_ref[...].astype(F32)
        sig = jax.nn.sigmoid(h1)
        silu = h1 * sig
        d1_ref[...] = (d_act * h3 * sig * (1.0 + h1 * (1.0 - sig))).astype(BF16)
        d3_ref[...] = (d_act * silu).astype(BF16)

    tile = pl.BlockSpec((row_tile, col_tile), lambda h, j, i, z_ref: (i, col(z_ref, h, j)))
    return pl.pallas_call(
        kernel,
        grid_spec=pltpu.PrefetchScalarGridSpec(
            num_scalar_prefetch=1,
            grid=(2, tiles, row_steps),
            in_specs=[
                pl.BlockSpec((rows, width), lambda h, j, i, z_ref: (0, 0)),
                pl.BlockSpec((col_tile, width), lambda h, j, i, z_ref: (jnp.where(h == 0, j, tiles - 1), 0)),
                pl.BlockSpec((col_tile, width), lambda h, j, i, z_ref: (jnp.where(h == 0, 0, j), 0)),
                tile, tile,
            ],
            out_specs=[tile] * 2,
        ),
        out_shape=[jax.ShapeDtypeStruct(h_gate.shape, BF16)] * 2,
        compiler_params=params('arbitrary', 'arbitrary', 'arbitrary'),
        cost_estimate=cost(2 * rows * width * 2 * half, 8 * rows * 2 * half),
    )(z, g_rows, w_own, w_other, h_gate, h_up)


def down_grad(which, h_gate, h_up, g_rows, halves, row_tile=512, col_tile=512):
    rows, cols = h_gate.shape
    width = g_rows.shape[1]
    tiles = cols // halves // col_tile

    def kernel(s_ref, h1_ref, h3_ref, g_ref, o_ref):
        i = pl.program_id(1)
        h1 = h1_ref[...].astype(F32)
        act = (h1 * jax.nn.sigmoid(h1) * h3_ref[...].astype(F32)).astype(BF16)
        g = g_ref[pl.ds(pl.multiple_of(i * row_tile, row_tile), row_tile), :]
        term = lax.dot_general(act, g, (((0,), (0,)), ((), ())), preferred_element_type=F32)

        @pl.when(i == 0)
        def _():
            o_ref[...] = term

        @pl.when(i > 0)
        def _():
            o_ref[...] += term

    tile = pl.BlockSpec((row_tile, col_tile), lambda j, i, s_ref: (i, s_ref[0] * tiles + j))
    return pl.pallas_call(
        kernel,
        grid_spec=pltpu.PrefetchScalarGridSpec(
            num_scalar_prefetch=1,
            grid=(tiles, rows // row_tile),
            in_specs=[tile, tile, pl.BlockSpec((rows, width), lambda j, i, s_ref: (0, 0))],
            out_specs=pl.BlockSpec((col_tile, width), lambda j, i, s_ref: (j, 0)),
        ),
        out_shape=jax.ShapeDtypeStruct((tiles * col_tile, width), F32),
        compiler_params=params('arbitrary', 'arbitrary'),
        cost_estimate=cost(2 * rows * width * tiles * col_tile, 4 * rows * cols),
    )(which, h_gate, h_up, g_rows)


def weight_grad_rhs(which, x_rows, wide, halves, col_tile=512):
    rows, cols = wide.shape
    part = x_rows.shape[1] // halves

    def kernel(s_ref, l_ref, r_ref, o_ref):
        o_ref[...] = lax.dot_general(l_ref[...], r_ref[...], (((0,), (0,)), ((), ())), preferred_element_type=F32)

    return pl.pallas_call(
        kernel,
        grid_spec=pltpu.PrefetchScalarGridSpec(
            num_scalar_prefetch=1,
            grid=(cols // col_tile,),
            in_specs=[
                pl.BlockSpec((rows, part), lambda j, s_ref: (0, s_ref[0])),
                pl.BlockSpec((rows, col_tile), lambda j, s_ref: (0, j)),
            ],
            out_specs=pl.BlockSpec((part, col_tile), lambda j, s_ref: (0, j)),
        ),
        out_shape=jax.ShapeDtypeStruct((part, cols), F32),
        compiler_params=params('arbitrary'),
        cost_estimate=cost(2 * rows * part * cols, 2 * rows * cols + 4 * part * cols),
    )(which, x_rows, wide)


def row_grads(z, dh_gate, dh_up, gate_own, gate_other, up_own, up_other, row_tile=256):
    rows, cols = dh_gate.shape
    part = gate_own.shape[0]

    def kernel(z_ref, d1_ref, d3_ref, g0_ref, g1_ref, u0_ref, u1_ref, o_ref):
        h = pl.program_id(0)
        dims = (((1,), (1,)), ((), ()))

        def emit(w1_ref, w3_ref):
            acc = lax.dot_general(d1_ref[...], w1_ref[...], dims, preferred_element_type=F32)
            acc += lax.dot_general(d3_ref[...], w3_ref[...], dims, preferred_element_type=F32)
            o_ref[...] = acc.astype(BF16)

        pl.when(h == 0)(lambda: emit(g0_ref, u0_ref))
        pl.when(h == 1)(lambda: emit(g1_ref, u1_ref))

    tile = pl.BlockSpec((row_tile, cols), lambda h, i, z_ref: (i, 0))
    full = pl.BlockSpec((part, cols), lambda h, i, z_ref: (0, 0))
    return pl.pallas_call(
        kernel,
        grid_spec=pltpu.PrefetchScalarGridSpec(
            num_scalar_prefetch=1,
            grid=(2, rows // row_tile),
            in_specs=[tile, tile, full, full, full, full],
            out_specs=pl.BlockSpec((row_tile, part), lambda h, i, z_ref: (i, jnp.where(h == 0, z_ref[0], 1 - z_ref[0]))),
        ),
        out_shape=jax.ShapeDtypeStruct((rows, 2 * part), BF16),
        compiler_params=params('arbitrary', 'arbitrary'),
        cost_estimate=cost(8 * rows * cols * part, 8 * rows * cols),
    )(z, dh_gate, dh_up, gate_own, gate_other, up_own, up_other)


def add_rows(own, recv, first, tile):
    rows, width = recv.shape
    base = first // tile

    def kernel(own_ref, recv_ref, o_ref):
        o_ref[...] = own_ref[...] + recv_ref[...]

    return pl.pallas_call(
        kernel,
        grid=(rows // tile,),
        in_specs=[pl.BlockSpec((tile, width), lambda i: (base + i, 0)), pl.BlockSpec((tile, width), lambda i: (i, 0))],
        out_specs=pl.BlockSpec((tile, width), lambda i: (base + i, 0)),
        out_shape=jax.ShapeDtypeStruct(own.shape, own.dtype),
        input_output_aliases={0: 0},
        compiler_params=params('arbitrary'),
        cost_estimate=cost(rows * width, 12 * rows * width),
    )(own, recv)


def add_piece(own, recv, first):
    rows, width = recv.shape

    def kernel(own_ref, recv_ref, o_ref, here, there, sem):
        place = pl.ds(first, rows)
        ins = (pltpu.make_async_copy(own_ref.at[place], here, sem.at[0]), pltpu.make_async_copy(recv_ref, there, sem.at[1]))
        for copy in ins:
            copy.start()
        for copy in ins:
            copy.wait()
        here[...] += there[...]
        out = pltpu.make_async_copy(here, o_ref.at[place], sem.at[2])
        out.start()
        out.wait()

    return pl.pallas_call(
        kernel,
        in_specs=[pl.BlockSpec(memory_space=pl.ANY)] * 2,
        out_specs=pl.BlockSpec(memory_space=pl.ANY),
        out_shape=jax.ShapeDtypeStruct(own.shape, own.dtype),
        scratch_shapes=[pltpu.VMEM((rows, width), F32)] * 2 + [pltpu.SemaphoreType.DMA((3,))],
        input_output_aliases={0: 0},
        compiler_params=params(),
        cost_estimate=cost(rows * width, 12 * rows * width),
    )(own, recv)


def add_last(own, tail, recv):
    rows, width = recv.shape
    first = own.shape[0] - rows

    def kernel(own_ref, tail_ref, recv_ref, o_ref, total, sem):
        total[...] = tail_ref[...] + recv_ref[...]
        out = pltpu.make_async_copy(total, o_ref.at[pl.ds(first, rows)], sem)
        out.start()
        out.wait()

    vmem = pl.BlockSpec(memory_space=pltpu.VMEM)
    return pl.pallas_call(
        kernel,
        in_specs=[pl.BlockSpec(memory_space=pl.ANY), vmem, vmem],
        out_specs=pl.BlockSpec(memory_space=pl.ANY),
        out_shape=jax.ShapeDtypeStruct(own.shape, own.dtype),
        scratch_shapes=[pltpu.VMEM((rows, width), F32), pltpu.SemaphoreType.DMA],
        input_output_aliases={0: 0},
        compiler_params=pltpu.CompilerParams(vmem_limit_bytes=4 * 1024 * 1024),
        cost_estimate=cost(rows * width, 12 * rows * width),
    )(own, pltpu.with_memory_space_constraint(tail, pltpu.VMEM), pltpu.with_memory_space_constraint(recv, pltpu.VMEM))


def solution(mesh):
    ep_n = mesh.shape['ep']
    fs_n = mesh.shape['fsdp']
    tok_spec = P(('fsdp', 'ep'), None)
    row_spec = P('ep', 'fsdp', None)
    swap = [(i, fs_n - 1 - i) for i in range(fs_n)]

    def exchange(value):
        return lax.ppermute(value, 'fsdp', swap)

    def local_backward(grad_out, expert_idx, slot_pos, gates, x_disp, h_gate, h_up, y_disp, w_gate, w_down, w_up):
        tok_n, top_n = expert_idx.shape
        e_loc, rows_loc, width = x_disp.shape
        slot_cap = rows_loc // ep_n
        slots_n = e_loc * ep_n * slot_cap
        choices = tok_n * top_n
        x_rows, y_rows, h_gate, h_up, w_gate, w_down, w_up = (v[0] for v in (x_disp, y_disp, h_gate, h_up, w_gate, w_down, w_up))

        z = lax.axis_index('fsdp').reshape(1).astype(jnp.int32)
        other_w_down = exchange(w_down)
        other_w_gate = exchange(w_gate)
        other_w_up = exchange(w_up)

        send_row = jnp.where(slot_pos >= 0, ((expert_idx % e_loc) * ep_n + expert_idx // e_loc) * slot_cap + slot_pos, slots_n).reshape(-1)
        src_choice = jnp.full((slots_n,), choices, jnp.int32).at[send_row].set(jnp.arange(choices, dtype=jnp.int32), mode='drop')
        send_dy = jnp.take(grad_out, src_choice // top_n, axis=0, mode='fill', fill_value=0).reshape(e_loc, ep_n, slot_cap, width)
        send_gate = jnp.take(gates.reshape(-1), src_choice, mode='fill', fill_value=0).reshape(e_loc, ep_n, slot_cap)
        dy_rows = lax.all_to_all(send_dy, 'ep', 1, 1, tiled=True).reshape(rows_loc, width)
        gate_rows = lax.all_to_all(send_gate, 'ep', 1, 1, tiled=True).reshape(rows_loc)
        g_rows = (dy_rows.astype(F32) * gate_rows[:, None]).astype(BF16)

        send = down_grad(1 - z, h_gate, h_up, g_rows, fs_n)
        recv_down = exchange(send)
        dh_gate, dh_up = hidden_grads(z, g_rows, w_down, other_w_down, h_gate, h_up)
        send = weight_grad_rhs(1 - z, x_rows, dh_gate, fs_n)
        recv_gate = exchange(send)
        send = weight_grad_rhs(1 - z, x_rows, dh_up, fs_n)
        step = send.shape[0] // 16
        cuts = (0, 12 * step, 15 * step + step // 3, 16 * step)
        recv_up = [exchange(send[lo:hi]) for lo, hi in zip(cuts, cuts[1:])]

        dx_rows = row_grads(z, dh_gate, dh_up, w_gate, other_w_gate, w_up, other_w_up)
        dgate_rows = jnp.einsum('rd,rd->r', dy_rows, y_rows, preferred_element_type=F32)
        back_dx = lax.all_to_all(dx_rows.reshape(e_loc, ep_n, slot_cap, width), 'ep', 1, 1, tiled=True).reshape(slots_n, width)
        back_gate = lax.all_to_all(dgate_rows.reshape(e_loc, ep_n, slot_cap), 'ep', 1, 1, tiled=True).reshape(slots_n)
        picked = jnp.take(back_dx, send_row, axis=0, mode='fill', fill_value=0).reshape(tok_n, top_n, width)
        grad_x = jnp.sum(picked.astype(F32), axis=1).astype(BF16)
        grad_gates = jnp.take(back_gate, send_row, mode='fill', fill_value=0).reshape(tok_n, top_n)

        grad_w_down = down_grad(z, h_gate, h_up, g_rows, fs_n)
        grad_w_gate = weight_grad_rhs(z, x_rows, dh_gate, fs_n)
        grad_w_up = weight_grad_rhs(z, x_rows, dh_up, fs_n)
        grad_w_down = add_rows(grad_w_down, recv_down, 0, 384)
        grad_w_gate = add_rows(grad_w_gate, recv_gate, 0, 4 * step)
        tail = grad_w_up[cuts[2]:]
        for n, recv in enumerate(recv_up[:-1]):
            grad_w_up = add_piece(grad_w_up, recv, cuts[n])
        grad_w_up = add_last(grad_w_up, tail, recv_up[-1])
        return grad_x, grad_gates, grad_w_gate[None], grad_w_down[None], grad_w_up[None]

    return jax.shard_map(local_backward, mesh=mesh, in_specs=(tok_spec, tok_spec, tok_spec, tok_spec, row_spec, row_spec, row_spec, row_spec, row_spec, row_spec, row_spec), out_specs=(tok_spec, tok_spec, row_spec, row_spec, row_spec), check_vma=False)
```

```python
import jax
import jax.numpy as jnp
from jax import lax
from jax.experimental import pallas as pl
from jax.experimental.pallas import tpu as pltpu
from jax.sharding import PartitionSpec as P


F32 = jnp.float32
BF16 = jnp.bfloat16
VMEM_LIMIT = 58 * 1024 * 1024


def params(*kinds):
    return pltpu.CompilerParams(dimension_semantics=kinds, vmem_limit_bytes=VMEM_LIMIT)


def cost(flops, bytes_accessed):
    return pl.CostEstimate(flops=flops, bytes_accessed=bytes_accessed, transcendentals=0)


def hidden_grads(z, g_rows, w_own, w_other, h_gate, h_up, row_tile=512, col_tile=512):
    rows, width = g_rows.shape
    half = w_own.shape[0]
    tiles = half // col_tile
    row_steps = rows // row_tile

    def col(z_ref, h, j):
        return jnp.where(h == 0, z_ref[0], 1 - z_ref[0]) * tiles + j

    def kernel(z_ref, g_ref, own_ref, other_ref, h1_ref, h3_ref, d1_ref, d3_ref):
        h, i = pl.program_id(0), pl.program_id(2)
        g = g_ref[pl.ds(pl.multiple_of(i * row_tile, row_tile), row_tile), :]
        w = jnp.where(h == 0, own_ref[...], other_ref[...])
        d_act = lax.dot_general(g, w, (((1,), (1,)), ((), ())), preferred_element_type=F32)
        h1 = h1_ref[...].astype(F32)
        h3 = h3_ref[...].astype(F32)
        sig = jax.nn.sigmoid(h1)
        silu = h1 * sig
        d1_ref[...] = (d_act * h3 * sig * (1.0 + h1 * (1.0 - sig))).astype(BF16)
        d3_ref[...] = (d_act * silu).astype(BF16)

    tile = pl.BlockSpec((row_tile, col_tile), lambda h, j, i, z_ref: (i, col(z_ref, h, j)))
    return pl.pallas_call(
        kernel,
        grid_spec=pltpu.PrefetchScalarGridSpec(
            num_scalar_prefetch=1,
            grid=(2, tiles, row_steps),
            in_specs=[
                pl.BlockSpec((rows, width), lambda h, j, i, z_ref: (0, 0)),
                pl.BlockSpec((col_tile, width), lambda h, j, i, z_ref: (jnp.where(h == 0, j, tiles - 1), 0)),
                pl.BlockSpec((col_tile, width), lambda h, j, i, z_ref: (jnp.where(h == 0, 0, j), 0)),
                tile, tile,
            ],
            out_specs=[tile] * 2,
        ),
        out_shape=[jax.ShapeDtypeStruct(h_gate.shape, BF16)] * 2,
        compiler_params=params('arbitrary', 'arbitrary', 'arbitrary'),
        cost_estimate=cost(2 * rows * width * 2 * half, 8 * rows * 2 * half),
    )(z, g_rows, w_own, w_other, h_gate, h_up)


def down_grad(which, h_gate, h_up, g_rows, halves, row_tile=512, col_tile=512):
    rows, cols = h_gate.shape
    width = g_rows.shape[1]
    tiles = cols // halves // col_tile

    def kernel(s_ref, h1_ref, h3_ref, g_ref, o_ref):
        i = pl.program_id(1)
        h1 = h1_ref[...].astype(F32)
        act = (h1 * jax.nn.sigmoid(h1) * h3_ref[...].astype(F32)).astype(BF16)
        g = g_ref[pl.ds(pl.multiple_of(i * row_tile, row_tile), row_tile), :]
        term = lax.dot_general(act, g, (((0,), (0,)), ((), ())), preferred_element_type=F32)

        @pl.when(i == 0)
        def _():
            o_ref[...] = term

        @pl.when(i > 0)
        def _():
            o_ref[...] += term

    tile = pl.BlockSpec((row_tile, col_tile), lambda j, i, s_ref: (i, s_ref[0] * tiles + j))
    return pl.pallas_call(
        kernel,
        grid_spec=pltpu.PrefetchScalarGridSpec(
            num_scalar_prefetch=1,
            grid=(tiles, rows // row_tile),
            in_specs=[tile, tile, pl.BlockSpec((rows, width), lambda j, i, s_ref: (0, 0))],
            out_specs=pl.BlockSpec((col_tile, width), lambda j, i, s_ref: (j, 0)),
        ),
        out_shape=jax.ShapeDtypeStruct((tiles * col_tile, width), F32),
        compiler_params=params('arbitrary', 'arbitrary'),
        cost_estimate=cost(2 * rows * width * tiles * col_tile, 4 * rows * cols),
    )(which, h_gate, h_up, g_rows)


def weight_grad_rhs(which, x_rows, wide, halves, col_tile=512):
    rows, cols = wide.shape
    part = x_rows.shape[1] // halves

    def kernel(s_ref, l_ref, r_ref, o_ref):
        o_ref[...] = lax.dot_general(l_ref[...], r_ref[...], (((0,), (0,)), ((), ())), preferred_element_type=F32)

    return pl.pallas_call(
        kernel,
        grid_spec=pltpu.PrefetchScalarGridSpec(
            num_scalar_prefetch=1,
            grid=(cols // col_tile,),
            in_specs=[
                pl.BlockSpec((rows, part), lambda j, s_ref: (0, s_ref[0])),
                pl.BlockSpec((rows, col_tile), lambda j, s_ref: (0, j)),
            ],
            out_specs=pl.BlockSpec((part, col_tile), lambda j, s_ref: (0, j)),
        ),
        out_shape=jax.ShapeDtypeStruct((part, cols), F32),
        compiler_params=params('arbitrary'),
        cost_estimate=cost(2 * rows * part * cols, 2 * rows * cols + 4 * part * cols),
    )(which, x_rows, wide)


def row_grads(z, dh_gate, dh_up, gate_own, gate_other, up_own, up_other, row_tile=256):
    rows, cols = dh_gate.shape
    part = gate_own.shape[0]

    def kernel(z_ref, d1_ref, d3_ref, g0_ref, g1_ref, u0_ref, u1_ref, o_ref):
        h = pl.program_id(0)
        dims = (((1,), (1,)), ((), ()))

        def emit(w1_ref, w3_ref):
            acc = lax.dot_general(d1_ref[...], w1_ref[...], dims, preferred_element_type=F32)
            acc += lax.dot_general(d3_ref[...], w3_ref[...], dims, preferred_element_type=F32)
            o_ref[...] = acc.astype(BF16)

        pl.when(h == 0)(lambda: emit(g0_ref, u0_ref))
        pl.when(h == 1)(lambda: emit(g1_ref, u1_ref))

    tile = pl.BlockSpec((row_tile, cols), lambda h, i, z_ref: (i, 0))
    full = pl.BlockSpec((part, cols), lambda h, i, z_ref: (0, 0))
    return pl.pallas_call(
        kernel,
        grid_spec=pltpu.PrefetchScalarGridSpec(
            num_scalar_prefetch=1,
            grid=(2, rows // row_tile),
            in_specs=[tile, tile, full, full, full, full],
            out_specs=pl.BlockSpec((row_tile, part), lambda h, i, z_ref: (i, jnp.where(h == 0, z_ref[0], 1 - z_ref[0]))),
        ),
        out_shape=jax.ShapeDtypeStruct((rows, 2 * part), BF16),
        compiler_params=params('arbitrary', 'arbitrary'),
        cost_estimate=cost(8 * rows * cols * part, 8 * rows * cols),
    )(z, dh_gate, dh_up, gate_own, gate_other, up_own, up_other)


def add_rows(own, recv, first, tile):
    rows, width = recv.shape
    base = first // tile

    def kernel(own_ref, recv_ref, o_ref):
        o_ref[...] = own_ref[...] + recv_ref[...]

    return pl.pallas_call(
        kernel,
        grid=(rows // tile,),
        in_specs=[pl.BlockSpec((tile, width), lambda i: (base + i, 0)), pl.BlockSpec((tile, width), lambda i: (i, 0))],
        out_specs=pl.BlockSpec((tile, width), lambda i: (base + i, 0)),
        out_shape=jax.ShapeDtypeStruct(own.shape, own.dtype),
        input_output_aliases={0: 0},
        compiler_params=params('arbitrary'),
        cost_estimate=cost(rows * width, 12 * rows * width),
    )(own, recv)


def add_piece(own, recv, first):
    rows, width = recv.shape

    def kernel(own_ref, recv_ref, o_ref, here, there, sem):
        place = pl.ds(first, rows)
        ins = (pltpu.make_async_copy(own_ref.at[place], here, sem.at[0]), pltpu.make_async_copy(recv_ref, there, sem.at[1]))
        for copy in ins:
            copy.start()
        for copy in ins:
            copy.wait()
        here[...] += there[...]
        out = pltpu.make_async_copy(here, o_ref.at[place], sem.at[2])
        out.start()
        out.wait()

    return pl.pallas_call(
        kernel,
        in_specs=[pl.BlockSpec(memory_space=pl.ANY)] * 2,
        out_specs=pl.BlockSpec(memory_space=pl.ANY),
        out_shape=jax.ShapeDtypeStruct(own.shape, own.dtype),
        scratch_shapes=[pltpu.VMEM((rows, width), F32)] * 2 + [pltpu.SemaphoreType.DMA((3,))],
        input_output_aliases={0: 0},
        compiler_params=params(),
        cost_estimate=cost(rows * width, 12 * rows * width),
    )(own, recv)


def add_last(own, tail, recv):
    rows, width = recv.shape
    first = own.shape[0] - rows

    def kernel(own_ref, tail_ref, recv_ref, o_ref, total, sem):
        total[...] = tail_ref[...] + recv_ref[...]
        out = pltpu.make_async_copy(total, o_ref.at[pl.ds(first, rows)], sem)
        out.start()
        out.wait()

    vmem = pl.BlockSpec(memory_space=pltpu.VMEM)
    return pl.pallas_call(
        kernel,
        in_specs=[pl.BlockSpec(memory_space=pl.ANY), vmem, vmem],
        out_specs=pl.BlockSpec(memory_space=pl.ANY),
        out_shape=jax.ShapeDtypeStruct(own.shape, own.dtype),
        scratch_shapes=[pltpu.VMEM((rows, width), F32), pltpu.SemaphoreType.DMA],
        input_output_aliases={0: 0},
        compiler_params=pltpu.CompilerParams(vmem_limit_bytes=4 * 1024 * 1024),
        cost_estimate=cost(rows * width, 12 * rows * width),
    )(own, pltpu.with_memory_space_constraint(tail, pltpu.VMEM), pltpu.with_memory_space_constraint(recv, pltpu.VMEM))


def solution(mesh):
    ep_n = mesh.shape['ep']
    fs_n = mesh.shape['fsdp']
    tok_spec = P(('fsdp', 'ep'), None)
    row_spec = P('ep', 'fsdp', None)
    swap = [(i, fs_n - 1 - i) for i in range(fs_n)]

    def exchange(value):
        return lax.ppermute(value, 'fsdp', swap)

    near = 2
    far = range(1, ep_n // near)

    def send(value, moves):
        return lax.ppermute(value, ('fsdp', 'ep'), [(a * ep_n + b, c * ep_n + d) for (a, b), (c, d) in moves])

    def detour(value):
        cols = value.shape[1] // len(far)
        grid = [(f, c) for f in range(fs_n) for c in range(near)]
        rest = [((f, e), (fs_n - 1 - f, e)) for f in range(fs_n) for e in range(near, ep_n)]
        out = [send(value[:, (k - 1) * cols:k * cols], [((f, c), (f, near * k + c)) for f, c in grid]) for k in far]
        crossed = send(sum(out[1:], out[0]), rest)
        direct = send(value, rest)
        back = [send(crossed, [((f, near * k + c), (f, c)) for f, c in grid]) for k in far]
        return direct, jnp.concatenate(back, axis=1)

    def local_backward(grad_out, expert_idx, slot_pos, gates, x_disp, h_gate, h_up, y_disp, w_gate, w_down, w_up):
        tok_n, top_n = expert_idx.shape
        e_loc, rows_loc, width = x_disp.shape
        slot_cap = rows_loc // ep_n
        slots_n = e_loc * ep_n * slot_cap
        choices = tok_n * top_n
        x_rows, y_rows, h_gate, h_up, w_gate, w_down, w_up = (v[0] for v in (x_disp, y_disp, h_gate, h_up, w_gate, w_down, w_up))

        z = lax.axis_index('fsdp').reshape(1).astype(jnp.int32)
        other_w_down = exchange(w_down)
        other_w_gate = exchange(w_gate)
        other_w_up = exchange(w_up)

        send_row = jnp.where(slot_pos >= 0, ((expert_idx % e_loc) * ep_n + expert_idx // e_loc) * slot_cap + slot_pos, slots_n).reshape(-1)
        src_choice = jnp.full((slots_n,), choices, jnp.int32).at[send_row].set(jnp.arange(choices, dtype=jnp.int32), mode='drop')
        send_dy = jnp.take(grad_out, src_choice // top_n, axis=0, mode='fill', fill_value=0).reshape(e_loc, ep_n, slot_cap, width)
        send_gate = jnp.take(gates.reshape(-1), src_choice, mode='fill', fill_value=0).reshape(e_loc, ep_n, slot_cap)
        dy_rows = lax.all_to_all(send_dy, 'ep', 1, 1, tiled=True).reshape(rows_loc, width)
        gate_rows = lax.all_to_all(send_gate, 'ep', 1, 1, tiled=True).reshape(rows_loc)
        g_rows = (dy_rows.astype(F32) * gate_rows[:, None]).astype(BF16)

        part = down_grad(1 - z, h_gate, h_up, g_rows, fs_n)
        recv_down = exchange(part)
        dh_gate, dh_up = hidden_grads(z, g_rows, w_down, other_w_down, h_gate, h_up)
        part = weight_grad_rhs(1 - z, x_rows, dh_gate, fs_n)
        recv_gate = exchange(part)
        send_up = weight_grad_rhs(1 - z, x_rows, dh_up, fs_n)
        step = send_up.shape[0] // 16
        cuts = (0, 12 * step, 15 * step, 15 * step + step // 3, 16 * step)
        piece = [send_up[lo:hi] for lo, hi in zip(cuts, cuts[1:])]
        direct, around = detour(piece[2])
        recv_up = [exchange(piece[0]), exchange(piece[1]), exchange(piece[3])]

        dx_rows = row_grads(z, dh_gate, dh_up, w_gate, other_w_gate, w_up, other_w_up)
        dgate_rows = jnp.einsum('rd,rd->r', dy_rows, y_rows, preferred_element_type=F32)
        back_dx = lax.all_to_all(dx_rows.reshape(e_loc, ep_n, slot_cap, width), 'ep', 1, 1, tiled=True).reshape(slots_n, width)
        back_gate = lax.all_to_all(dgate_rows.reshape(e_loc, ep_n, slot_cap), 'ep', 1, 1, tiled=True).reshape(slots_n)
        picked = jnp.take(back_dx, send_row, axis=0, mode='fill', fill_value=0).reshape(tok_n, top_n, width)
        grad_x = jnp.sum(picked.astype(F32), axis=1).astype(BF16)
        grad_gates = jnp.take(back_gate, send_row, mode='fill', fill_value=0).reshape(tok_n, top_n)

        grad_w_down = down_grad(z, h_gate, h_up, g_rows, fs_n)
        grad_w_gate = weight_grad_rhs(z, x_rows, dh_gate, fs_n)
        grad_w_up = weight_grad_rhs(z, x_rows, dh_up, fs_n)
        grad_w_down = add_rows(grad_w_down, recv_down, 0, 384)
        grad_w_gate = add_rows(grad_w_gate, recv_gate, 0, 4 * step)
        tail = grad_w_up[cuts[3]:]
        grad_w_up = add_piece(grad_w_up, recv_up[0], cuts[0])
        grad_w_up = add_piece(grad_w_up, direct + around, cuts[2])
        grad_w_up = add_piece(grad_w_up, recv_up[1], cuts[1])
        grad_w_up = add_last(grad_w_up, tail, recv_up[-1])
        return grad_x, grad_gates, grad_w_gate[None], grad_w_down[None], grad_w_up[None]

    return jax.shard_map(local_backward, mesh=mesh, in_specs=(tok_spec, tok_spec, tok_spec, tok_spec, row_spec, row_spec, row_spec, row_spec, row_spec, row_spec, row_spec), out_specs=(tok_spec, tok_spec, row_spec, row_spec, row_spec), check_vma=False)
```

```python
import jax
import jax.numpy as jnp
from jax import lax
from jax.experimental import pallas as pl
from jax.experimental.pallas import tpu as pltpu
from jax.sharding import PartitionSpec as P


F32 = jnp.float32
BF16 = jnp.bfloat16
VMEM_LIMIT = 58 * 1024 * 1024


def params(*kinds):
    return pltpu.CompilerParams(dimension_semantics=kinds, vmem_limit_bytes=VMEM_LIMIT)


def cost(flops, bytes_accessed):
    return pl.CostEstimate(flops=flops, bytes_accessed=bytes_accessed, transcendentals=0)


def hidden_grads(z, g_rows, w_own, w_other, h_gate, h_up, row_tile=512, col_tile=512):
    rows, width = g_rows.shape
    half = w_own.shape[0]
    tiles = half // col_tile
    row_steps = rows // row_tile

    def col(z_ref, h, j):
        return jnp.where(h == 0, z_ref[0], 1 - z_ref[0]) * tiles + j

    def kernel(z_ref, g_ref, own_ref, other_ref, h1_ref, h3_ref, d1_ref, d3_ref):
        h, i = pl.program_id(0), pl.program_id(2)
        g = g_ref[pl.ds(pl.multiple_of(i * row_tile, row_tile), row_tile), :]
        w = jnp.where(h == 0, own_ref[...], other_ref[...])
        d_act = lax.dot_general(g, w, (((1,), (1,)), ((), ())), preferred_element_type=F32)
        h1 = h1_ref[...].astype(F32)
        h3 = h3_ref[...].astype(F32)
        sig = jax.nn.sigmoid(h1)
        silu = h1 * sig
        d1_ref[...] = (d_act * h3 * sig * (1.0 + h1 * (1.0 - sig))).astype(BF16)
        d3_ref[...] = (d_act * silu).astype(BF16)

    tile = pl.BlockSpec((row_tile, col_tile), lambda h, j, i, z_ref: (i, col(z_ref, h, j)))
    return pl.pallas_call(
        kernel,
        grid_spec=pltpu.PrefetchScalarGridSpec(
            num_scalar_prefetch=1,
            grid=(2, tiles, row_steps),
            in_specs=[
                pl.BlockSpec((rows, width), lambda h, j, i, z_ref: (0, 0)),
                pl.BlockSpec((col_tile, width), lambda h, j, i, z_ref: (jnp.where(h == 0, j, tiles - 1), 0)),
                pl.BlockSpec((col_tile, width), lambda h, j, i, z_ref: (jnp.where(h == 0, 0, j), 0)),
                tile, tile,
            ],
            out_specs=[tile] * 2,
        ),
        out_shape=[jax.ShapeDtypeStruct(h_gate.shape, BF16)] * 2,
        compiler_params=params('arbitrary', 'arbitrary', 'arbitrary'),
        cost_estimate=cost(2 * rows * width * 2 * half, 8 * rows * 2 * half),
    )(z, g_rows, w_own, w_other, h_gate, h_up)


def down_grad(which, h_gate, h_up, g_rows, halves, row_tile=512, col_tile=512):
    rows, cols = h_gate.shape
    width = g_rows.shape[1]
    tiles = cols // halves // col_tile

    def kernel(s_ref, h1_ref, h3_ref, g_ref, o_ref):
        i = pl.program_id(1)
        h1 = h1_ref[...].astype(F32)
        act = (h1 * jax.nn.sigmoid(h1) * h3_ref[...].astype(F32)).astype(BF16)
        g = g_ref[pl.ds(pl.multiple_of(i * row_tile, row_tile), row_tile), :]
        term = lax.dot_general(act, g, (((0,), (0,)), ((), ())), preferred_element_type=F32)

        @pl.when(i == 0)
        def _():
            o_ref[...] = term

        @pl.when(i > 0)
        def _():
            o_ref[...] += term

    tile = pl.BlockSpec((row_tile, col_tile), lambda j, i, s_ref: (i, s_ref[0] * tiles + j))
    return pl.pallas_call(
        kernel,
        grid_spec=pltpu.PrefetchScalarGridSpec(
            num_scalar_prefetch=1,
            grid=(tiles, rows // row_tile),
            in_specs=[tile, tile, pl.BlockSpec((rows, width), lambda j, i, s_ref: (0, 0))],
            out_specs=pl.BlockSpec((col_tile, width), lambda j, i, s_ref: (j, 0)),
        ),
        out_shape=jax.ShapeDtypeStruct((tiles * col_tile, width), F32),
        compiler_params=params('arbitrary', 'arbitrary'),
        cost_estimate=cost(2 * rows * width * tiles * col_tile, 4 * rows * cols),
    )(which, h_gate, h_up, g_rows)


def weight_grad_rhs(which, x_rows, wide, halves, col_tile=512):
    rows, cols = wide.shape
    part = x_rows.shape[1] // halves

    def kernel(s_ref, l_ref, r_ref, o_ref):
        o_ref[...] = lax.dot_general(l_ref[...], r_ref[...], (((0,), (0,)), ((), ())), preferred_element_type=F32)

    return pl.pallas_call(
        kernel,
        grid_spec=pltpu.PrefetchScalarGridSpec(
            num_scalar_prefetch=1,
            grid=(cols // col_tile,),
            in_specs=[
                pl.BlockSpec((rows, part), lambda j, s_ref: (0, s_ref[0])),
                pl.BlockSpec((rows, col_tile), lambda j, s_ref: (0, j)),
            ],
            out_specs=pl.BlockSpec((part, col_tile), lambda j, s_ref: (0, j)),
        ),
        out_shape=jax.ShapeDtypeStruct((part, cols), F32),
        compiler_params=params('arbitrary'),
        cost_estimate=cost(2 * rows * part * cols, 2 * rows * cols + 4 * part * cols),
    )(which, x_rows, wide)


def row_grads(z, dh_gate, dh_up, gate_own, gate_other, up_own, up_other, row_tile=256):
    rows, cols = dh_gate.shape
    part = gate_own.shape[0]

    def kernel(z_ref, d1_ref, d3_ref, g0_ref, g1_ref, u0_ref, u1_ref, o_ref):
        h = pl.program_id(0)
        dims = (((1,), (1,)), ((), ()))

        def emit(w1_ref, w3_ref):
            acc = lax.dot_general(d1_ref[...], w1_ref[...], dims, preferred_element_type=F32)
            acc += lax.dot_general(d3_ref[...], w3_ref[...], dims, preferred_element_type=F32)
            o_ref[...] = acc.astype(BF16)

        pl.when(h == 0)(lambda: emit(g0_ref, u0_ref))
        pl.when(h == 1)(lambda: emit(g1_ref, u1_ref))

    tile = pl.BlockSpec((row_tile, cols), lambda h, i, z_ref: (i, 0))
    full = pl.BlockSpec((part, cols), lambda h, i, z_ref: (0, 0))
    return pl.pallas_call(
        kernel,
        grid_spec=pltpu.PrefetchScalarGridSpec(
            num_scalar_prefetch=1,
            grid=(2, rows // row_tile),
            in_specs=[tile, tile, full, full, full, full],
            out_specs=pl.BlockSpec((row_tile, part), lambda h, i, z_ref: (i, jnp.where(h == 0, z_ref[0], 1 - z_ref[0]))),
        ),
        out_shape=jax.ShapeDtypeStruct((rows, 2 * part), BF16),
        compiler_params=params('arbitrary', 'arbitrary'),
        cost_estimate=cost(8 * rows * cols * part, 8 * rows * cols),
    )(z, dh_gate, dh_up, gate_own, gate_other, up_own, up_other)


def add_rows(own, recv, first, tile):
    rows, width = recv.shape
    base = first // tile

    def kernel(own_ref, recv_ref, o_ref):
        o_ref[...] = own_ref[...] + recv_ref[...]

    return pl.pallas_call(
        kernel,
        grid=(rows // tile,),
        in_specs=[pl.BlockSpec((tile, width), lambda i: (base + i, 0)), pl.BlockSpec((tile, width), lambda i: (i, 0))],
        out_specs=pl.BlockSpec((tile, width), lambda i: (base + i, 0)),
        out_shape=jax.ShapeDtypeStruct(own.shape, own.dtype),
        input_output_aliases={0: 0},
        compiler_params=params('arbitrary'),
        cost_estimate=cost(rows * width, 12 * rows * width),
    )(own, recv)


def add_piece(own, recv, first):
    rows, width = recv.shape

    def kernel(own_ref, recv_ref, o_ref, here, there, sem):
        place = pl.ds(first, rows)
        ins = (pltpu.make_async_copy(own_ref.at[place], here, sem.at[0]), pltpu.make_async_copy(recv_ref, there, sem.at[1]))
        for copy in ins:
            copy.start()
        for copy in ins:
            copy.wait()
        here[...] += there[...]
        out = pltpu.make_async_copy(here, o_ref.at[place], sem.at[2])
        out.start()
        out.wait()

    return pl.pallas_call(
        kernel,
        in_specs=[pl.BlockSpec(memory_space=pl.ANY)] * 2,
        out_specs=pl.BlockSpec(memory_space=pl.ANY),
        out_shape=jax.ShapeDtypeStruct(own.shape, own.dtype),
        scratch_shapes=[pltpu.VMEM((rows, width), F32)] * 2 + [pltpu.SemaphoreType.DMA((3,))],
        input_output_aliases={0: 0},
        compiler_params=params(),
        cost_estimate=cost(rows * width, 12 * rows * width),
    )(own, recv)


def add_last(own, tail, recv):
    rows, width = recv.shape
    first = own.shape[0] - rows

    def kernel(own_ref, tail_ref, recv_ref, o_ref, total, sem):
        total[...] = tail_ref[...] + recv_ref[...]
        out = pltpu.make_async_copy(total, o_ref.at[pl.ds(first, rows)], sem)
        out.start()
        out.wait()

    vmem = pl.BlockSpec(memory_space=pltpu.VMEM)
    return pl.pallas_call(
        kernel,
        in_specs=[pl.BlockSpec(memory_space=pl.ANY), vmem, vmem],
        out_specs=pl.BlockSpec(memory_space=pl.ANY),
        out_shape=jax.ShapeDtypeStruct(own.shape, own.dtype),
        scratch_shapes=[pltpu.VMEM((rows, width), F32), pltpu.SemaphoreType.DMA],
        input_output_aliases={0: 0},
        compiler_params=pltpu.CompilerParams(vmem_limit_bytes=4 * 1024 * 1024),
        cost_estimate=cost(rows * width, 12 * rows * width),
    )(own, pltpu.with_memory_space_constraint(tail, pltpu.VMEM), pltpu.with_memory_space_constraint(recv, pltpu.VMEM))


def solution(mesh):
    ep_n = mesh.shape['ep']
    fs_n = mesh.shape['fsdp']
    tok_spec = P(('fsdp', 'ep'), None)
    row_spec = P('ep', 'fsdp', None)
    swap = [(i, fs_n - 1 - i) for i in range(fs_n)]

    def exchange(value):
        return lax.ppermute(value, 'fsdp', swap)

    near = 2
    chips = ep_n // near
    odd = [near * k + 1 for k in range(chips)]

    def send(value, moves):
        return lax.ppermute(value, ('fsdp', 'ep'), [(f * ep_n + a, g * ep_n + b) for f in range(fs_n) for a, b, g in moves(f)])

    def within(pairs):
        return lambda f: [(a, b, f) for a, b in pairs]

    def across(devices):
        return lambda f: [(e, e, fs_n - 1 - f) for e in devices]

    def balanced(value):
        third = value.shape[1] * 5 // 24
        cut = value.shape[1] - 3 * third
        side, long = value[:, :cut], value[:, cut:]
        handed = send(side, within([(e - 1, e) for e in odd]))
        parts = [send(long[:, n * third:(n + 1) * third], within([(0, e)])) for n, e in enumerate(odd[1:])]
        handed = send(handed, across(odd))
        passed = send(sum(parts[1:], parts[0]), across(odd[1:]))
        own_side = send(side, across(odd))
        own_long = send(long, across(range(1, ep_n)))
        handed = send(handed, within([(e, e - 1) for e in odd]))
        back = [send(passed, within([(e, 0)])) for e in odd[1:]]
        return own_side, handed, own_long, back

    def local_backward(grad_out, expert_idx, slot_pos, gates, x_disp, h_gate, h_up, y_disp, w_gate, w_down, w_up):
        tok_n, top_n = expert_idx.shape
        e_loc, rows_loc, width = x_disp.shape
        slot_cap = rows_loc // ep_n
        slots_n = e_loc * ep_n * slot_cap
        choices = tok_n * top_n
        x_rows, y_rows, h_gate, h_up, w_gate, w_down, w_up = (v[0] for v in (x_disp, y_disp, h_gate, h_up, w_gate, w_down, w_up))

        z = lax.axis_index('fsdp').reshape(1).astype(jnp.int32)
        other_w_down = exchange(w_down)
        other_w_gate = exchange(w_gate)
        other_w_up = exchange(w_up)

        send_row = jnp.where(slot_pos >= 0, ((expert_idx % e_loc) * ep_n + expert_idx // e_loc) * slot_cap + slot_pos, slots_n).reshape(-1)
        src_choice = jnp.full((slots_n,), choices, jnp.int32).at[send_row].set(jnp.arange(choices, dtype=jnp.int32), mode='drop')
        send_dy = jnp.take(grad_out, src_choice // top_n, axis=0, mode='fill', fill_value=0).reshape(e_loc, ep_n, slot_cap, width)
        send_gate = jnp.take(gates.reshape(-1), src_choice, mode='fill', fill_value=0).reshape(e_loc, ep_n, slot_cap)
        dy_rows = lax.all_to_all(send_dy, 'ep', 1, 1, tiled=True).reshape(rows_loc, width)
        gate_rows = lax.all_to_all(send_gate, 'ep', 1, 1, tiled=True).reshape(rows_loc)
        g_rows = (dy_rows.astype(F32) * gate_rows[:, None]).astype(BF16)

        part = down_grad(1 - z, h_gate, h_up, g_rows, fs_n)
        recv_down = exchange(part)
        dh_gate, dh_up = hidden_grads(z, g_rows, w_down, other_w_down, h_gate, h_up)
        part = weight_grad_rhs(1 - z, x_rows, dh_gate, fs_n)
        recv_gate = exchange(part)
        send_up = weight_grad_rhs(1 - z, x_rows, dh_up, fs_n)
        step = send_up.shape[0] // 16
        cuts = (0, 12 * step, 15 * step, 15 * step + step // 3, 16 * step)
        piece = [send_up[lo:hi] for lo, hi in zip(cuts, cuts[1:])]
        own_side, handed, own_long, back = balanced(piece[2])
        recv_up = [exchange(piece[0]), exchange(piece[1]), exchange(piece[3])]

        dx_rows = row_grads(z, dh_gate, dh_up, w_gate, other_w_gate, w_up, other_w_up)
        dgate_rows = jnp.einsum('rd,rd->r', dy_rows, y_rows, preferred_element_type=F32)
        back_dx = lax.all_to_all(dx_rows.reshape(e_loc, ep_n, slot_cap, width), 'ep', 1, 1, tiled=True).reshape(slots_n, width)
        back_gate = lax.all_to_all(dgate_rows.reshape(e_loc, ep_n, slot_cap), 'ep', 1, 1, tiled=True).reshape(slots_n)
        picked = jnp.take(back_dx, send_row, axis=0, mode='fill', fill_value=0).reshape(tok_n, top_n, width)
        grad_x = jnp.sum(picked.astype(F32), axis=1).astype(BF16)
        grad_gates = jnp.take(back_gate, send_row, mode='fill', fill_value=0).reshape(tok_n, top_n)

        grad_w_down = down_grad(z, h_gate, h_up, g_rows, fs_n)
        grad_w_gate = weight_grad_rhs(z, x_rows, dh_gate, fs_n)
        grad_w_up = weight_grad_rhs(z, x_rows, dh_up, fs_n)
        grad_w_down = add_rows(grad_w_down, recv_down, 0, 384)
        grad_w_gate = add_rows(grad_w_gate, recv_gate, 0, 4 * step)
        tail = grad_w_up[cuts[3]:]
        grad_w_up = add_piece(grad_w_up, recv_up[0], cuts[0])
        band = jnp.concatenate([own_side + handed, own_long + jnp.concatenate(back, axis=1)], axis=1)
        grad_w_up = add_piece(grad_w_up, band, cuts[2])
        grad_w_up = add_piece(grad_w_up, recv_up[1], cuts[1])
        grad_w_up = add_last(grad_w_up, tail, recv_up[-1])
        return grad_x, grad_gates, grad_w_gate[None], grad_w_down[None], grad_w_up[None]

    return jax.shard_map(local_backward, mesh=mesh, in_specs=(tok_spec, tok_spec, tok_spec, tok_spec, row_spec, row_spec, row_spec, row_spec, row_spec, row_spec, row_spec), out_specs=(tok_spec, tok_spec, row_spec, row_spec, row_spec), check_vma=False)
```

```python
import jax
import jax.numpy as jnp
from jax import lax
from jax.experimental import pallas as pl
from jax.experimental.pallas import tpu as pltpu
from jax.sharding import PartitionSpec as P


F32 = jnp.float32
BF16 = jnp.bfloat16
VMEM_LIMIT = 58 * 1024 * 1024


def params(*kinds):
    return pltpu.CompilerParams(dimension_semantics=kinds, vmem_limit_bytes=VMEM_LIMIT)


def cost(flops, bytes_accessed):
    return pl.CostEstimate(flops=flops, bytes_accessed=bytes_accessed, transcendentals=0)


def hidden_grads(z, g_rows, w_own, w_other, h_gate, h_up, row_tile=512, col_tile=512):
    rows, width = g_rows.shape
    half = w_own.shape[0]
    tiles = half // col_tile
    row_steps = rows // row_tile

    def col(z_ref, h, j):
        return jnp.where(h == 0, z_ref[0], 1 - z_ref[0]) * tiles + j

    def kernel(z_ref, g_ref, own_ref, other_ref, h1_ref, h3_ref, d1_ref, d3_ref):
        h, i = pl.program_id(0), pl.program_id(2)
        g = g_ref[pl.ds(pl.multiple_of(i * row_tile, row_tile), row_tile), :]
        w = jnp.where(h == 0, own_ref[...], other_ref[...])
        d_act = lax.dot_general(g, w, (((1,), (1,)), ((), ())), preferred_element_type=F32)
        h1 = h1_ref[...].astype(F32)
        h3 = h3_ref[...].astype(F32)
        sig = jax.nn.sigmoid(h1)
        silu = h1 * sig
        d1_ref[...] = (d_act * h3 * sig * (1.0 + h1 * (1.0 - sig))).astype(BF16)
        d3_ref[...] = (d_act * silu).astype(BF16)

    tile = pl.BlockSpec((row_tile, col_tile), lambda h, j, i, z_ref: (i, col(z_ref, h, j)))
    return pl.pallas_call(
        kernel,
        grid_spec=pltpu.PrefetchScalarGridSpec(
            num_scalar_prefetch=1,
            grid=(2, tiles, row_steps),
            in_specs=[
                pl.BlockSpec((rows, width), lambda h, j, i, z_ref: (0, 0)),
                pl.BlockSpec((col_tile, width), lambda h, j, i, z_ref: (jnp.where(h == 0, j, tiles - 1), 0)),
                pl.BlockSpec((col_tile, width), lambda h, j, i, z_ref: (jnp.where(h == 0, 0, j), 0)),
                tile, tile,
            ],
            out_specs=[tile] * 2,
        ),
        out_shape=[jax.ShapeDtypeStruct(h_gate.shape, BF16)] * 2,
        compiler_params=params('arbitrary', 'arbitrary', 'arbitrary'),
        cost_estimate=cost(2 * rows * width * 2 * half, 8 * rows * 2 * half),
    )(z, g_rows, w_own, w_other, h_gate, h_up)


def down_grad(which, h_gate, h_up, g_rows, halves, row_tile=512, col_tile=512):
    rows, cols = h_gate.shape
    width = g_rows.shape[1]
    tiles = cols // halves // col_tile

    def kernel(s_ref, h1_ref, h3_ref, g_ref, o_ref):
        i = pl.program_id(1)
        h1 = h1_ref[...].astype(F32)
        act = (h1 * jax.nn.sigmoid(h1) * h3_ref[...].astype(F32)).astype(BF16)
        g = g_ref[pl.ds(pl.multiple_of(i * row_tile, row_tile), row_tile), :]
        term = lax.dot_general(act, g, (((0,), (0,)), ((), ())), preferred_element_type=F32)

        @pl.when(i == 0)
        def _():
            o_ref[...] = term

        @pl.when(i > 0)
        def _():
            o_ref[...] += term

    tile = pl.BlockSpec((row_tile, col_tile), lambda j, i, s_ref: (i, s_ref[0] * tiles + j))
    return pl.pallas_call(
        kernel,
        grid_spec=pltpu.PrefetchScalarGridSpec(
            num_scalar_prefetch=1,
            grid=(tiles, rows // row_tile),
            in_specs=[tile, tile, pl.BlockSpec((rows, width), lambda j, i, s_ref: (0, 0))],
            out_specs=pl.BlockSpec((col_tile, width), lambda j, i, s_ref: (j, 0)),
        ),
        out_shape=jax.ShapeDtypeStruct((tiles * col_tile, width), F32),
        compiler_params=params('arbitrary', 'arbitrary'),
        cost_estimate=cost(2 * rows * width * tiles * col_tile, 4 * rows * cols),
    )(which, h_gate, h_up, g_rows)


def weight_grad_rhs(which, x_rows, wide, halves, col_tile=512):
    rows, cols = wide.shape
    part = x_rows.shape[1] // halves

    def kernel(s_ref, l_ref, r_ref, o_ref):
        o_ref[...] = lax.dot_general(l_ref[...], r_ref[...], (((0,), (0,)), ((), ())), preferred_element_type=F32)

    return pl.pallas_call(
        kernel,
        grid_spec=pltpu.PrefetchScalarGridSpec(
            num_scalar_prefetch=1,
            grid=(cols // col_tile,),
            in_specs=[
                pl.BlockSpec((rows, part), lambda j, s_ref: (0, s_ref[0])),
                pl.BlockSpec((rows, col_tile), lambda j, s_ref: (0, j)),
            ],
            out_specs=pl.BlockSpec((part, col_tile), lambda j, s_ref: (0, j)),
        ),
        out_shape=jax.ShapeDtypeStruct((part, cols), F32),
        compiler_params=params('arbitrary'),
        cost_estimate=cost(2 * rows * part * cols, 2 * rows * cols + 4 * part * cols),
    )(which, x_rows, wide)


def row_grads(z, dh_gate, dh_up, gate_own, gate_other, up_own, up_other, row_tile=256):
    rows, cols = dh_gate.shape
    part = gate_own.shape[0]

    def kernel(z_ref, d1_ref, d3_ref, g0_ref, g1_ref, u0_ref, u1_ref, o_ref):
        h = pl.program_id(0)
        dims = (((1,), (1,)), ((), ()))

        def emit(w1_ref, w3_ref):
            acc = lax.dot_general(d1_ref[...], w1_ref[...], dims, preferred_element_type=F32)
            acc += lax.dot_general(d3_ref[...], w3_ref[...], dims, preferred_element_type=F32)
            o_ref[...] = acc.astype(BF16)

        pl.when(h == 0)(lambda: emit(g0_ref, u0_ref))
        pl.when(h == 1)(lambda: emit(g1_ref, u1_ref))

    tile = pl.BlockSpec((row_tile, cols), lambda h, i, z_ref: (i, 0))
    full = pl.BlockSpec((part, cols), lambda h, i, z_ref: (0, 0))
    return pl.pallas_call(
        kernel,
        grid_spec=pltpu.PrefetchScalarGridSpec(
            num_scalar_prefetch=1,
            grid=(2, rows // row_tile),
            in_specs=[tile, tile, full, full, full, full],
            out_specs=pl.BlockSpec((row_tile, part), lambda h, i, z_ref: (i, jnp.where(h == 0, z_ref[0], 1 - z_ref[0]))),
        ),
        out_shape=jax.ShapeDtypeStruct((rows, 2 * part), BF16),
        compiler_params=params('arbitrary', 'arbitrary'),
        cost_estimate=cost(8 * rows * cols * part, 8 * rows * cols),
    )(z, dh_gate, dh_up, gate_own, gate_other, up_own, up_other)


def add_rows(own, recv, first, tile):
    rows, width = recv.shape
    base = first // tile

    def kernel(own_ref, recv_ref, o_ref):
        o_ref[...] = own_ref[...] + recv_ref[...]

    return pl.pallas_call(
        kernel,
        grid=(rows // tile,),
        in_specs=[pl.BlockSpec((tile, width), lambda i: (base + i, 0)), pl.BlockSpec((tile, width), lambda i: (i, 0))],
        out_specs=pl.BlockSpec((tile, width), lambda i: (base + i, 0)),
        out_shape=jax.ShapeDtypeStruct(own.shape, own.dtype),
        input_output_aliases={0: 0},
        compiler_params=params('arbitrary'),
        cost_estimate=cost(rows * width, 12 * rows * width),
    )(own, recv)


def add_piece(own, recv, first):
    rows, width = recv.shape

    def kernel(own_ref, recv_ref, o_ref, here, there, sem):
        place = pl.ds(first, rows)
        ins = (pltpu.make_async_copy(own_ref.at[place], here, sem.at[0]), pltpu.make_async_copy(recv_ref, there, sem.at[1]))
        for copy in ins:
            copy.start()
        for copy in ins:
            copy.wait()
        here[...] += there[...]
        out = pltpu.make_async_copy(here, o_ref.at[place], sem.at[2])
        out.start()
        out.wait()

    return pl.pallas_call(
        kernel,
        in_specs=[pl.BlockSpec(memory_space=pl.ANY)] * 2,
        out_specs=pl.BlockSpec(memory_space=pl.ANY),
        out_shape=jax.ShapeDtypeStruct(own.shape, own.dtype),
        scratch_shapes=[pltpu.VMEM((rows, width), F32)] * 2 + [pltpu.SemaphoreType.DMA((3,))],
        input_output_aliases={0: 0},
        compiler_params=params(),
        cost_estimate=cost(rows * width, 12 * rows * width),
    )(own, recv)


def add_last(own, tail, recv):
    rows, width = recv.shape
    first = own.shape[0] - rows

    def kernel(own_ref, tail_ref, recv_ref, o_ref, total, sem):
        total[...] = tail_ref[...] + recv_ref[...]
        out = pltpu.make_async_copy(total, o_ref.at[pl.ds(first, rows)], sem)
        out.start()
        out.wait()

    vmem = pl.BlockSpec(memory_space=pltpu.VMEM)
    return pl.pallas_call(
        kernel,
        in_specs=[pl.BlockSpec(memory_space=pl.ANY), vmem, vmem],
        out_specs=pl.BlockSpec(memory_space=pl.ANY),
        out_shape=jax.ShapeDtypeStruct(own.shape, own.dtype),
        scratch_shapes=[pltpu.VMEM((rows, width), F32), pltpu.SemaphoreType.DMA],
        input_output_aliases={0: 0},
        compiler_params=pltpu.CompilerParams(vmem_limit_bytes=4 * 1024 * 1024),
        cost_estimate=cost(rows * width, 12 * rows * width),
    )(own, pltpu.with_memory_space_constraint(tail, pltpu.VMEM), pltpu.with_memory_space_constraint(recv, pltpu.VMEM))


def solution(mesh):
    ep_n = mesh.shape['ep']
    fs_n = mesh.shape['fsdp']
    tok_spec = P(('fsdp', 'ep'), None)
    row_spec = P('ep', 'fsdp', None)
    swap = [(i, fs_n - 1 - i) for i in range(fs_n)]

    def exchange(value):
        return lax.ppermute(value, 'fsdp', swap)

    near = 2
    far = range(1, ep_n // near)

    def send(value, moves):
        return lax.ppermute(value, ('fsdp', 'ep'), [(a * ep_n + b, c * ep_n + d) for (a, b), (c, d) in moves])

    def detour(value):
        cols = value.shape[1] // len(far)
        grid = [(f, c) for f in range(fs_n) for c in range(near)]
        rest = [((f, e), (fs_n - 1 - f, e)) for f in range(fs_n) for e in range(near, ep_n)]
        out = [send(value[:, (k - 1) * cols:k * cols], [((f, c), (f, near * k + c)) for f, c in grid]) for k in far]
        crossed = send(sum(out[1:], out[0]), rest)
        direct = send(value, rest)
        back = [send(crossed, [((f, near * k + c), (f, c)) for f, c in grid]) for k in far]
        return direct, jnp.concatenate(back, axis=1)

    def local_backward(grad_out, expert_idx, slot_pos, gates, x_disp, h_gate, h_up, y_disp, w_gate, w_down, w_up):
        tok_n, top_n = expert_idx.shape
        e_loc, rows_loc, width = x_disp.shape
        slot_cap = rows_loc // ep_n
        slots_n = e_loc * ep_n * slot_cap
        choices = tok_n * top_n
        x_rows, y_rows, h_gate, h_up, w_gate, w_down, w_up = (v[0] for v in (x_disp, y_disp, h_gate, h_up, w_gate, w_down, w_up))

        z = lax.axis_index('fsdp').reshape(1).astype(jnp.int32)
        other_w_down = exchange(w_down)
        other_w_gate = exchange(w_gate)
        other_w_up = exchange(w_up)

        send_row = jnp.where(slot_pos >= 0, ((expert_idx % e_loc) * ep_n + expert_idx // e_loc) * slot_cap + slot_pos, slots_n).reshape(-1)
        src_choice = jnp.full((slots_n,), choices, jnp.int32).at[send_row].set(jnp.arange(choices, dtype=jnp.int32), mode='drop')
        send_dy = jnp.take(grad_out, src_choice // top_n, axis=0, mode='fill', fill_value=0).reshape(e_loc, ep_n, slot_cap, width)
        send_gate = jnp.take(gates.reshape(-1), src_choice, mode='fill', fill_value=0).reshape(e_loc, ep_n, slot_cap)
        dy_rows = lax.all_to_all(send_dy, 'ep', 1, 1, tiled=True).reshape(rows_loc, width)
        gate_rows = lax.all_to_all(send_gate, 'ep', 1, 1, tiled=True).reshape(rows_loc)
        g_rows = (dy_rows.astype(F32) * gate_rows[:, None]).astype(BF16)

        part = down_grad(1 - z, h_gate, h_up, g_rows, fs_n)
        recv_down = exchange(part)
        dh_gate, dh_up = hidden_grads(z, g_rows, w_down, other_w_down, h_gate, h_up)
        part = weight_grad_rhs(1 - z, x_rows, dh_gate, fs_n)
        recv_gate = exchange(part)
        send_up = weight_grad_rhs(1 - z, x_rows, dh_up, fs_n)
        step = send_up.shape[0] // 16
        cuts = (0, 12 * step + step // 3, 15 * step, 15 * step + step // 3, 16 * step)
        piece = [send_up[lo:hi] for lo, hi in zip(cuts, cuts[1:])]
        half = piece[2].shape[1] // 2
        direct, around = detour(piece[2][:, :half])
        plain = exchange(piece[2][:, half:])
        recv_up = [exchange(piece[0]), exchange(piece[1]), exchange(piece[3])]

        dx_rows = row_grads(z, dh_gate, dh_up, w_gate, other_w_gate, w_up, other_w_up)
        dgate_rows = jnp.einsum('rd,rd->r', dy_rows, y_rows, preferred_element_type=F32)
        back_dx = lax.all_to_all(dx_rows.reshape(e_loc, ep_n, slot_cap, width), 'ep', 1, 1, tiled=True).reshape(slots_n, width)
        back_gate = lax.all_to_all(dgate_rows.reshape(e_loc, ep_n, slot_cap), 'ep', 1, 1, tiled=True).reshape(slots_n)
        picked = jnp.take(back_dx, send_row, axis=0, mode='fill', fill_value=0).reshape(tok_n, top_n, width)
        grad_x = jnp.sum(picked.astype(F32), axis=1).astype(BF16)
        grad_gates = jnp.take(back_gate, send_row, mode='fill', fill_value=0).reshape(tok_n, top_n)

        grad_w_down = down_grad(z, h_gate, h_up, g_rows, fs_n)
        grad_w_gate = weight_grad_rhs(z, x_rows, dh_gate, fs_n)
        grad_w_up = weight_grad_rhs(z, x_rows, dh_up, fs_n)
        grad_w_down = add_rows(grad_w_down, recv_down, 0, 384)
        grad_w_gate = add_rows(grad_w_gate, recv_gate, 0, 4 * step)
        tail = grad_w_up[cuts[3]:]
        grad_w_up = add_piece(grad_w_up, recv_up[0], cuts[0])
        grad_w_up = add_piece(grad_w_up, jnp.concatenate([direct + around, plain], axis=1), cuts[2])
        grad_w_up = add_piece(grad_w_up, recv_up[1], cuts[1])
        grad_w_up = add_last(grad_w_up, tail, recv_up[-1])
        return grad_x, grad_gates, grad_w_gate[None], grad_w_down[None], grad_w_up[None]

    return jax.shard_map(local_backward, mesh=mesh, in_specs=(tok_spec, tok_spec, tok_spec, tok_spec, row_spec, row_spec, row_spec, row_spec, row_spec, row_spec, row_spec), out_specs=(tok_spec, tok_spec, row_spec, row_spec, row_spec), check_vma=False)
```

```python
import jax
import jax.numpy as jnp
from jax import lax
from jax.experimental import pallas as pl
from jax.experimental.pallas import tpu as pltpu
from jax.sharding import PartitionSpec as P


F32 = jnp.float32
BF16 = jnp.bfloat16
VMEM_LIMIT = 58 * 1024 * 1024


def params(*kinds):
    return pltpu.CompilerParams(dimension_semantics=kinds, vmem_limit_bytes=VMEM_LIMIT)


def cost(flops, bytes_accessed):
    return pl.CostEstimate(flops=flops, bytes_accessed=bytes_accessed, transcendentals=0)


def hidden_grads(z, g_rows, w_own, w_other, h_gate, h_up, row_tile=1280, col_tile=512):
    rows, width = g_rows.shape
    half = w_own.shape[0]
    tiles = half // col_tile
    row_steps = rows // row_tile

    def col(z_ref, h, j):
        return jnp.where(h == 0, z_ref[0], 1 - z_ref[0]) * tiles + j

    def kernel(z_ref, g_ref, own_ref, other_ref, h1_ref, h3_ref, d1_ref, d3_ref):
        h, i = pl.program_id(0), pl.program_id(2)
        g = g_ref[pl.ds(pl.multiple_of(i * row_tile, row_tile), row_tile), :]
        w = jnp.where(h == 0, own_ref[...], other_ref[...])
        d_act = lax.dot_general(g, w, (((1,), (1,)), ((), ())), preferred_element_type=F32)
        h1 = h1_ref[...].astype(F32)
        h3 = h3_ref[...].astype(F32)
        sig = jax.nn.sigmoid(h1)
        silu = h1 * sig
        d1_ref[...] = (d_act * h3 * sig * (1.0 + h1 * (1.0 - sig))).astype(BF16)
        d3_ref[...] = (d_act * silu).astype(BF16)

    tile = pl.BlockSpec((row_tile, col_tile), lambda h, j, i, z_ref: (i, col(z_ref, h, j)))
    return pl.pallas_call(
        kernel,
        grid_spec=pltpu.PrefetchScalarGridSpec(
            num_scalar_prefetch=1,
            grid=(2, tiles, row_steps),
            in_specs=[
                pl.BlockSpec((rows, width), lambda h, j, i, z_ref: (0, 0)),
                pl.BlockSpec((col_tile, width), lambda h, j, i, z_ref: (jnp.where(h == 0, j, tiles - 1), 0)),
                pl.BlockSpec((col_tile, width), lambda h, j, i, z_ref: (jnp.where(h == 0, 0, j), 0)),
                tile, tile,
            ],
            out_specs=[tile] * 2,
        ),
        out_shape=[jax.ShapeDtypeStruct(h_gate.shape, BF16)] * 2,
        compiler_params=params('arbitrary', 'arbitrary', 'arbitrary'),
        cost_estimate=cost(2 * rows * width * 2 * half, 8 * rows * 2 * half),
    )(z, g_rows, w_own, w_other, h_gate, h_up)


def down_grad(which, h_gate, h_up, g_rows, halves, row_tile=1280, col_tile=512):
    rows, cols = h_gate.shape
    width = g_rows.shape[1]
    tiles = cols // halves // col_tile

    def kernel(s_ref, h1_ref, h3_ref, g_ref, o_ref):
        i = pl.program_id(1)
        h1 = h1_ref[...].astype(F32)
        act = (h1 * jax.nn.sigmoid(h1) * h3_ref[...].astype(F32)).astype(BF16)
        g = g_ref[pl.ds(pl.multiple_of(i * row_tile, row_tile), row_tile), :]
        term = lax.dot_general(act, g, (((0,), (0,)), ((), ())), preferred_element_type=F32)

        @pl.when(i == 0)
        def _():
            o_ref[...] = term

        @pl.when(i > 0)
        def _():
            o_ref[...] += term

    tile = pl.BlockSpec((row_tile, col_tile), lambda j, i, s_ref: (i, s_ref[0] * tiles + j))
    return pl.pallas_call(
        kernel,
        grid_spec=pltpu.PrefetchScalarGridSpec(
            num_scalar_prefetch=1,
            grid=(tiles, rows // row_tile),
            in_specs=[tile, tile, pl.BlockSpec((rows, width), lambda j, i, s_ref: (0, 0))],
            out_specs=pl.BlockSpec((col_tile, width), lambda j, i, s_ref: (j, 0)),
        ),
        out_shape=jax.ShapeDtypeStruct((tiles * col_tile, width), F32),
        compiler_params=params('arbitrary', 'arbitrary'),
        cost_estimate=cost(2 * rows * width * tiles * col_tile, 4 * rows * cols),
    )(which, h_gate, h_up, g_rows)


def weight_grad_rhs(which, x_rows, wide, halves, cuts=(), col_tile=1024):
    rows, cols = wide.shape
    part = x_rows.shape[1] // halves
    cuts = cuts or (0, part)
    spans = list(zip(cuts, cuts[1:]))

    def kernel(s_ref, l_ref, r_ref, *o_refs):
        total = lax.dot_general(l_ref[...], r_ref[...], (((0,), (0,)), ((), ())), preferred_element_type=F32)
        for o_ref, (lo, hi) in zip(o_refs, spans):
            o_ref[...] = total[lo:hi]

    return pl.pallas_call(
        kernel,
        grid_spec=pltpu.PrefetchScalarGridSpec(
            num_scalar_prefetch=1,
            grid=(cols // col_tile,),
            in_specs=[
                pl.BlockSpec((rows, part), lambda j, s_ref: (0, s_ref[0])),
                pl.BlockSpec((rows, col_tile), lambda j, s_ref: (0, j)),
            ],
            out_specs=[pl.BlockSpec((hi - lo, col_tile), lambda j, s_ref: (0, j)) for lo, hi in spans],
        ),
        out_shape=[jax.ShapeDtypeStruct((hi - lo, cols), F32) for lo, hi in spans],
        compiler_params=params('arbitrary'),
        cost_estimate=cost(2 * rows * part * cols, 2 * rows * cols + 4 * part * cols),
    )(which, x_rows, wide)


def row_grads(z, dh_gate, dh_up, gate_own, gate_other, up_own, up_other, row_tile=640):
    rows, cols = dh_gate.shape
    part = gate_own.shape[0]

    def kernel(z_ref, d1_ref, d3_ref, g0_ref, g1_ref, u0_ref, u1_ref, o_ref):
        h = pl.program_id(0)
        dims = (((1,), (1,)), ((), ()))

        def emit(w1_ref, w3_ref):
            acc = lax.dot_general(d1_ref[...], w1_ref[...], dims, preferred_element_type=F32)
            acc += lax.dot_general(d3_ref[...], w3_ref[...], dims, preferred_element_type=F32)
            o_ref[...] = acc.astype(BF16)

        pl.when(h == 0)(lambda: emit(g0_ref, u0_ref))
        pl.when(h == 1)(lambda: emit(g1_ref, u1_ref))

    tile = pl.BlockSpec((row_tile, cols), lambda h, i, z_ref: (i, 0))
    full = pl.BlockSpec((part, cols), lambda h, i, z_ref: (0, 0))
    return pl.pallas_call(
        kernel,
        grid_spec=pltpu.PrefetchScalarGridSpec(
            num_scalar_prefetch=1,
            grid=(2, rows // row_tile),
            in_specs=[tile, tile, full, full, full, full],
            out_specs=pl.BlockSpec((row_tile, part), lambda h, i, z_ref: (i, jnp.where(h == 0, z_ref[0], 1 - z_ref[0]))),
        ),
        out_shape=jax.ShapeDtypeStruct((rows, 2 * part), BF16),
        compiler_params=params('arbitrary', 'arbitrary'),
        cost_estimate=cost(8 * rows * cols * part, 8 * rows * cols),
    )(z, dh_gate, dh_up, gate_own, gate_other, up_own, up_other)


def add_rows(own, recv, first, tile):
    rows, width = recv.shape
    base = first // tile

    def kernel(own_ref, recv_ref, o_ref):
        o_ref[...] = own_ref[...] + recv_ref[...]

    return pl.pallas_call(
        kernel,
        grid=(rows // tile,),
        in_specs=[pl.BlockSpec((tile, width), lambda i: (base + i, 0)), pl.BlockSpec((tile, width), lambda i: (i, 0))],
        out_specs=pl.BlockSpec((tile, width), lambda i: (base + i, 0)),
        out_shape=jax.ShapeDtypeStruct(own.shape, own.dtype),
        input_output_aliases={0: 0},
        compiler_params=params('arbitrary'),
        cost_estimate=cost(rows * width, 12 * rows * width),
    )(own, recv)


def add_piece(own, recv, first):
    rows, width = recv.shape

    def kernel(own_ref, recv_ref, o_ref, here, there, sem):
        place = pl.ds(first, rows)
        ins = (pltpu.make_async_copy(own_ref.at[place], here, sem.at[0]), pltpu.make_async_copy(recv_ref, there, sem.at[1]))
        for copy in ins:
            copy.start()
        for copy in ins:
            copy.wait()
        here[...] += there[...]
        out = pltpu.make_async_copy(here, o_ref.at[place], sem.at[2])
        out.start()
        out.wait()

    return pl.pallas_call(
        kernel,
        in_specs=[pl.BlockSpec(memory_space=pl.ANY)] * 2,
        out_specs=pl.BlockSpec(memory_space=pl.ANY),
        out_shape=jax.ShapeDtypeStruct(own.shape, own.dtype),
        scratch_shapes=[pltpu.VMEM((rows, width), F32)] * 2 + [pltpu.SemaphoreType.DMA((3,))],
        input_output_aliases={0: 0},
        compiler_params=params(),
        cost_estimate=cost(rows * width, 12 * rows * width),
    )(own, recv)


def add_last(own, tail, recv):
    rows, width = recv.shape
    first = own.shape[0] - rows

    def kernel(own_ref, tail_ref, recv_ref, o_ref, total, sem):
        total[...] = tail_ref[...] + recv_ref[...]
        out = pltpu.make_async_copy(total, o_ref.at[pl.ds(first, rows)], sem)
        out.start()
        out.wait()

    vmem = pl.BlockSpec(memory_space=pltpu.VMEM)
    return pl.pallas_call(
        kernel,
        in_specs=[pl.BlockSpec(memory_space=pl.ANY), vmem, vmem],
        out_specs=pl.BlockSpec(memory_space=pl.ANY),
        out_shape=jax.ShapeDtypeStruct(own.shape, own.dtype),
        scratch_shapes=[pltpu.VMEM((rows, width), F32), pltpu.SemaphoreType.DMA],
        input_output_aliases={0: 0},
        compiler_params=pltpu.CompilerParams(vmem_limit_bytes=4 * 1024 * 1024),
        cost_estimate=cost(rows * width, 12 * rows * width),
    )(own, pltpu.with_memory_space_constraint(tail, pltpu.VMEM), pltpu.with_memory_space_constraint(recv, pltpu.VMEM))


def solution(mesh):
    ep_n = mesh.shape['ep']
    fs_n = mesh.shape['fsdp']
    tok_spec = P(('fsdp', 'ep'), None)
    row_spec = P('ep', 'fsdp', None)
    swap = [(i, fs_n - 1 - i) for i in range(fs_n)]

    def exchange(value):
        return lax.ppermute(value, 'fsdp', swap)

    near = 2
    far = range(1, ep_n // near)

    def send(value, moves):
        return lax.ppermute(value, ('fsdp', 'ep'), [(a * ep_n + b, c * ep_n + d) for (a, b), (c, d) in moves])

    def detour(value):
        cols = value.shape[1] // len(far)
        grid = [(f, c) for f in range(fs_n) for c in range(near)]
        rest = [((f, e), (fs_n - 1 - f, e)) for f in range(fs_n) for e in range(near, ep_n)]
        out = [send(value[:, (k - 1) * cols:k * cols], [((f, c), (f, near * k + c)) for f, c in grid]) for k in far]
        crossed = send(sum(out[1:], out[0]), rest)
        direct = send(value, rest)
        back = [send(crossed, [((f, near * k + c), (f, c)) for f, c in grid]) for k in far]
        return direct, jnp.concatenate(back, axis=1)

    def local_backward(grad_out, expert_idx, slot_pos, gates, x_disp, h_gate, h_up, y_disp, w_gate, w_down, w_up):
        tok_n, top_n = expert_idx.shape
        e_loc, rows_loc, width = x_disp.shape
        slot_cap = rows_loc // ep_n
        slots_n = e_loc * ep_n * slot_cap
        choices = tok_n * top_n
        x_rows, y_rows, h_gate, h_up, w_gate, w_down, w_up = (v[0] for v in (x_disp, y_disp, h_gate, h_up, w_gate, w_down, w_up))

        z = lax.axis_index('fsdp').reshape(1).astype(jnp.int32)
        other_w_down = exchange(w_down)
        other_w_gate = exchange(w_gate)
        other_w_up = exchange(w_up)

        send_row = jnp.where(slot_pos >= 0, ((expert_idx % e_loc) * ep_n + expert_idx // e_loc) * slot_cap + slot_pos, slots_n).reshape(-1)
        src_choice = jnp.full((slots_n,), choices, jnp.int32).at[send_row].set(jnp.arange(choices, dtype=jnp.int32), mode='drop')
        send_dy = jnp.take(grad_out, src_choice // top_n, axis=0, mode='fill', fill_value=0).reshape(e_loc, ep_n, slot_cap, width)
        send_gate = jnp.take(gates.reshape(-1), src_choice, mode='fill', fill_value=0).reshape(e_loc, ep_n, slot_cap)
        dy_rows = lax.all_to_all(send_dy, 'ep', 1, 1, tiled=True).reshape(rows_loc, width)
        gate_rows = lax.all_to_all(send_gate, 'ep', 1, 1, tiled=True).reshape(rows_loc)
        g_rows = (dy_rows.astype(F32) * gate_rows[:, None]).astype(BF16)

        part = down_grad(1 - z, h_gate, h_up, g_rows, fs_n)
        recv_down = exchange(part)
        dh_gate, dh_up = hidden_grads(z, g_rows, w_down, other_w_down, h_gate, h_up)
        part, = weight_grad_rhs(1 - z, x_rows, dh_gate, fs_n)
        recv_gate = exchange(part)
        step = width // fs_n // 16
        cuts = (0, 12 * step + step // 3, 15 * step, 15 * step + step // 3, 16 * step)
        piece = weight_grad_rhs(1 - z, x_rows, dh_up, fs_n, cuts)
        half = piece[2].shape[1] // 2
        direct, around = detour(piece[2][:, :half])
        plain = exchange(piece[2][:, half:])
        recv_up = [exchange(piece[0]), exchange(piece[1]), exchange(piece[3])]

        dx_rows = row_grads(z, dh_gate, dh_up, w_gate, other_w_gate, w_up, other_w_up)
        dgate_rows = jnp.einsum('rd,rd->r', dy_rows, y_rows, preferred_element_type=F32)
        back_dx = lax.all_to_all(dx_rows.reshape(e_loc, ep_n, slot_cap, width), 'ep', 1, 1, tiled=True).reshape(slots_n, width)
        back_gate = lax.all_to_all(dgate_rows.reshape(e_loc, ep_n, slot_cap), 'ep', 1, 1, tiled=True).reshape(slots_n)
        picked = jnp.take(back_dx, send_row, axis=0, mode='fill', fill_value=0).reshape(tok_n, top_n, width)
        grad_x = jnp.sum(picked.astype(F32), axis=1).astype(BF16)
        grad_gates = jnp.take(back_gate, send_row, mode='fill', fill_value=0).reshape(tok_n, top_n)

        grad_w_down = down_grad(z, h_gate, h_up, g_rows, fs_n)
        grad_w_gate, = weight_grad_rhs(z, x_rows, dh_gate, fs_n)
        grad_w_up, = weight_grad_rhs(z, x_rows, dh_up, fs_n)
        grad_w_down = add_rows(grad_w_down, recv_down, 0, 768)
        grad_w_gate = add_rows(grad_w_gate, recv_gate, 0, 8 * step)
        tail = grad_w_up[cuts[3]:]
        grad_w_up = add_piece(grad_w_up, recv_up[0], cuts[0])
        grad_w_up = add_piece(grad_w_up, jnp.concatenate([direct + around, plain], axis=1), cuts[2])
        grad_w_up = add_piece(grad_w_up, recv_up[1], cuts[1])
        grad_w_up = add_last(grad_w_up, tail, recv_up[-1])
        return grad_x, grad_gates, grad_w_gate[None], grad_w_down[None], grad_w_up[None]

    return jax.shard_map(local_backward, mesh=mesh, in_specs=(tok_spec, tok_spec, tok_spec, tok_spec, row_spec, row_spec, row_spec, row_spec, row_spec, row_spec, row_spec), out_specs=(tok_spec, tok_spec, row_spec, row_spec, row_spec), check_vma=False)
```

```python
import jax
import jax.numpy as jnp
from jax import lax
from jax.experimental import pallas as pl
from jax.experimental.pallas import tpu as pltpu
from jax.sharding import PartitionSpec as P


F32 = jnp.float32
BF16 = jnp.bfloat16
VMEM_LIMIT = 58 * 1024 * 1024


def params(*kinds):
    return pltpu.CompilerParams(dimension_semantics=kinds, vmem_limit_bytes=VMEM_LIMIT)


def cost(flops, bytes_accessed):
    return pl.CostEstimate(flops=flops, bytes_accessed=bytes_accessed, transcendentals=0)


def hidden_grads(z, g_rows, w_own, w_other, h_gate, h_up, row_tile=1280, col_tile=512):
    rows, width = g_rows.shape
    half = w_own.shape[0]
    tiles = half // col_tile
    row_steps = rows // row_tile

    def col(z_ref, h, j):
        return jnp.where(h == 0, z_ref[0], 1 - z_ref[0]) * tiles + j

    def kernel(z_ref, g_ref, own_ref, other_ref, h1_ref, h3_ref, d1_ref, d3_ref):
        h, i = pl.program_id(0), pl.program_id(2)
        g = g_ref[pl.ds(pl.multiple_of(i * row_tile, row_tile), row_tile), :]
        w = jnp.where(h == 0, own_ref[...], other_ref[...])
        d_act = lax.dot_general(g, w, (((1,), (1,)), ((), ())), preferred_element_type=F32)
        h1 = h1_ref[...].astype(F32)
        h3 = h3_ref[...].astype(F32)
        sig = jax.nn.sigmoid(h1)
        silu = h1 * sig
        d1_ref[...] = (d_act * h3 * sig * (1.0 + h1 * (1.0 - sig))).astype(BF16)
        d3_ref[...] = (d_act * silu).astype(BF16)

    tile = pl.BlockSpec((row_tile, col_tile), lambda h, j, i, z_ref: (i, col(z_ref, h, j)))
    return pl.pallas_call(
        kernel,
        grid_spec=pltpu.PrefetchScalarGridSpec(
            num_scalar_prefetch=1,
            grid=(2, tiles, row_steps),
            in_specs=[
                pl.BlockSpec((rows, width), lambda h, j, i, z_ref: (0, 0)),
                pl.BlockSpec((col_tile, width), lambda h, j, i, z_ref: (jnp.where(h == 0, j, tiles - 1), 0)),
                pl.BlockSpec((col_tile, width), lambda h, j, i, z_ref: (jnp.where(h == 0, 0, j), 0)),
                tile, tile,
            ],
            out_specs=[tile] * 2,
        ),
        out_shape=[jax.ShapeDtypeStruct(h_gate.shape, BF16)] * 2,
        compiler_params=params('arbitrary', 'arbitrary', 'arbitrary'),
        cost_estimate=cost(2 * rows * width * 2 * half, 8 * rows * 2 * half),
    )(z, g_rows, w_own, w_other, h_gate, h_up)


def down_grad(which, h_gate, h_up, g_rows, halves, recv=None, row_tile=1280, col_tile=512):
    rows, cols = h_gate.shape
    width = g_rows.shape[1]
    tiles = cols // halves // col_tile
    steps = rows // row_tile
    extra = [] if recv is None else [recv]

    def kernel(s_ref, h1_ref, h3_ref, g_ref, *refs):
        o_ref = refs[-1]
        i = pl.program_id(1)
        h1 = h1_ref[...].astype(F32)
        act = (h1 * jax.nn.sigmoid(h1) * h3_ref[...].astype(F32)).astype(BF16)
        g = g_ref[pl.ds(pl.multiple_of(i * row_tile, row_tile), row_tile), :]
        term = lax.dot_general(act, g, (((0,), (0,)), ((), ())), preferred_element_type=F32)

        @pl.when(i == 0)
        def _():
            o_ref[...] = term

        @pl.when(i > 0)
        def _():
            o_ref[...] += term

        if extra:
            @pl.when(i == steps - 1)
            def _():
                o_ref[...] += refs[0][...]

    out_tile = pl.BlockSpec((col_tile, width), lambda j, i, s_ref: (j, 0))
    tile = pl.BlockSpec((row_tile, col_tile), lambda j, i, s_ref: (i, s_ref[0] * tiles + j))
    return pl.pallas_call(
        kernel,
        grid_spec=pltpu.PrefetchScalarGridSpec(
            num_scalar_prefetch=1,
            grid=(tiles, steps),
            in_specs=[tile, tile, pl.BlockSpec((rows, width), lambda j, i, s_ref: (0, 0))] + [out_tile] * len(extra),
            out_specs=out_tile,
        ),
        out_shape=jax.ShapeDtypeStruct((tiles * col_tile, width), F32),
        compiler_params=params('arbitrary', 'arbitrary'),
        cost_estimate=cost(2 * rows * width * tiles * col_tile, 4 * rows * cols),
    )(which, h_gate, h_up, g_rows, *extra)


def weight_grad_rhs(which, x_rows, wide, halves, cuts=(), recv=None, col_tile=1024):
    rows, cols = wide.shape
    part = x_rows.shape[1] // halves
    cuts = cuts or (0, part)
    spans = list(zip(cuts, cuts[1:]))
    extra = [] if recv is None else [recv]

    def kernel(s_ref, l_ref, r_ref, *refs):
        o_refs = refs[len(extra):]
        total = lax.dot_general(l_ref[...], r_ref[...], (((0,), (0,)), ((), ())), preferred_element_type=F32)
        for o_ref, (lo, hi) in zip(o_refs, spans):
            o_ref[...] = total[lo:hi]
        if extra:
            o_refs[0][:recv.shape[0], :] += refs[0][...]

    return pl.pallas_call(
        kernel,
        grid_spec=pltpu.PrefetchScalarGridSpec(
            num_scalar_prefetch=1,
            grid=(cols // col_tile,),
            in_specs=[
                pl.BlockSpec((rows, part), lambda j, s_ref: (0, s_ref[0])),
                pl.BlockSpec((rows, col_tile), lambda j, s_ref: (0, j)),
            ] + [pl.BlockSpec((v.shape[0], col_tile), lambda j, s_ref: (0, j)) for v in extra],
            out_specs=[pl.BlockSpec((hi - lo, col_tile), lambda j, s_ref: (0, j)) for lo, hi in spans],
        ),
        out_shape=[jax.ShapeDtypeStruct((hi - lo, cols), F32) for lo, hi in spans],
        compiler_params=params('arbitrary'),
        cost_estimate=cost(2 * rows * part * cols, 2 * rows * cols + 4 * part * cols),
    )(which, x_rows, wide, *extra)


def row_grads(z, dh_gate, dh_up, gate_own, gate_other, up_own, up_other, row_tile=640):
    rows, cols = dh_gate.shape
    part = gate_own.shape[0]

    def kernel(z_ref, d1_ref, d3_ref, g0_ref, g1_ref, u0_ref, u1_ref, o_ref):
        h = pl.program_id(0)
        dims = (((1,), (1,)), ((), ()))

        def emit(w1_ref, w3_ref):
            acc = lax.dot_general(d1_ref[...], w1_ref[...], dims, preferred_element_type=F32)
            acc += lax.dot_general(d3_ref[...], w3_ref[...], dims, preferred_element_type=F32)
            o_ref[...] = acc.astype(BF16)

        pl.when(h == 0)(lambda: emit(g0_ref, u0_ref))
        pl.when(h == 1)(lambda: emit(g1_ref, u1_ref))

    tile = pl.BlockSpec((row_tile, cols), lambda h, i, z_ref: (i, 0))
    full = pl.BlockSpec((part, cols), lambda h, i, z_ref: (0, 0))
    return pl.pallas_call(
        kernel,
        grid_spec=pltpu.PrefetchScalarGridSpec(
            num_scalar_prefetch=1,
            grid=(2, rows // row_tile),
            in_specs=[tile, tile, full, full, full, full],
            out_specs=pl.BlockSpec((row_tile, part), lambda h, i, z_ref: (i, jnp.where(h == 0, z_ref[0], 1 - z_ref[0]))),
        ),
        out_shape=jax.ShapeDtypeStruct((rows, 2 * part), BF16),
        compiler_params=params('arbitrary', 'arbitrary'),
        cost_estimate=cost(8 * rows * cols * part, 8 * rows * cols),
    )(z, dh_gate, dh_up, gate_own, gate_other, up_own, up_other)


def add_piece(own, recv, first):
    rows, width = recv.shape

    def kernel(own_ref, recv_ref, o_ref, here, there, sem):
        place = pl.ds(first, rows)
        ins = (pltpu.make_async_copy(own_ref.at[place], here, sem.at[0]), pltpu.make_async_copy(recv_ref, there, sem.at[1]))
        for copy in ins:
            copy.start()
        for copy in ins:
            copy.wait()
        here[...] += there[...]
        out = pltpu.make_async_copy(here, o_ref.at[place], sem.at[2])
        out.start()
        out.wait()

    return pl.pallas_call(
        kernel,
        in_specs=[pl.BlockSpec(memory_space=pl.ANY)] * 2,
        out_specs=pl.BlockSpec(memory_space=pl.ANY),
        out_shape=jax.ShapeDtypeStruct(own.shape, own.dtype),
        scratch_shapes=[pltpu.VMEM((rows, width), F32)] * 2 + [pltpu.SemaphoreType.DMA((3,))],
        input_output_aliases={0: 0},
        compiler_params=params(),
        cost_estimate=cost(rows * width, 12 * rows * width),
    )(own, recv)


def add_last(own, tail, recv):
    rows, width = recv.shape
    first = own.shape[0] - rows

    def kernel(own_ref, tail_ref, recv_ref, o_ref, total, sem):
        total[...] = tail_ref[...] + recv_ref[...]
        out = pltpu.make_async_copy(total, o_ref.at[pl.ds(first, rows)], sem)
        out.start()
        out.wait()

    vmem = pl.BlockSpec(memory_space=pltpu.VMEM)
    return pl.pallas_call(
        kernel,
        in_specs=[pl.BlockSpec(memory_space=pl.ANY), vmem, vmem],
        out_specs=pl.BlockSpec(memory_space=pl.ANY),
        out_shape=jax.ShapeDtypeStruct(own.shape, own.dtype),
        scratch_shapes=[pltpu.VMEM((rows, width), F32), pltpu.SemaphoreType.DMA],
        input_output_aliases={0: 0},
        compiler_params=pltpu.CompilerParams(vmem_limit_bytes=4 * 1024 * 1024),
        cost_estimate=cost(rows * width, 12 * rows * width),
    )(own, pltpu.with_memory_space_constraint(tail, pltpu.VMEM), pltpu.with_memory_space_constraint(recv, pltpu.VMEM))


def solution(mesh):
    ep_n = mesh.shape['ep']
    fs_n = mesh.shape['fsdp']
    tok_spec = P(('fsdp', 'ep'), None)
    row_spec = P('ep', 'fsdp', None)
    swap = [(i, fs_n - 1 - i) for i in range(fs_n)]

    def exchange(value):
        return lax.ppermute(value, 'fsdp', swap)

    near = 2
    far = range(1, ep_n // near)

    def send(value, moves):
        return lax.ppermute(value, ('fsdp', 'ep'), [(a * ep_n + b, c * ep_n + d) for (a, b), (c, d) in moves])

    def detour(value):
        cols = value.shape[1] // len(far)
        grid = [(f, c) for f in range(fs_n) for c in range(near)]
        rest = [((f, e), (fs_n - 1 - f, e)) for f in range(fs_n) for e in range(near, ep_n)]
        out = [send(value[:, (k - 1) * cols:k * cols], [((f, c), (f, near * k + c)) for f, c in grid]) for k in far]
        crossed = send(sum(out[1:], out[0]), rest)
        direct = send(value, rest)
        back = [send(crossed, [((f, near * k + c), (f, c)) for f, c in grid]) for k in far]
        return direct, jnp.concatenate(back, axis=1)

    def local_backward(grad_out, expert_idx, slot_pos, gates, x_disp, h_gate, h_up, y_disp, w_gate, w_down, w_up):
        tok_n, top_n = expert_idx.shape
        e_loc, rows_loc, width = x_disp.shape
        slot_cap = rows_loc // ep_n
        slots_n = e_loc * ep_n * slot_cap
        choices = tok_n * top_n
        x_rows, y_rows, h_gate, h_up, w_gate, w_down, w_up = (v[0] for v in (x_disp, y_disp, h_gate, h_up, w_gate, w_down, w_up))

        z = lax.axis_index('fsdp').reshape(1).astype(jnp.int32)
        other_w_down = exchange(w_down)
        other_w_gate = exchange(w_gate)
        other_w_up = exchange(w_up)

        send_row = jnp.where(slot_pos >= 0, ((expert_idx % e_loc) * ep_n + expert_idx // e_loc) * slot_cap + slot_pos, slots_n).reshape(-1)
        src_choice = jnp.full((slots_n,), choices, jnp.int32).at[send_row].set(jnp.arange(choices, dtype=jnp.int32), mode='drop')
        send_dy = jnp.take(grad_out, src_choice // top_n, axis=0, mode='clip').reshape(e_loc, ep_n, slot_cap, width)
        send_gate = jnp.take(gates.reshape(-1), src_choice, mode='fill', fill_value=0).reshape(e_loc, ep_n, slot_cap)
        dy_rows = lax.all_to_all(send_dy, 'ep', 1, 1, tiled=True).reshape(rows_loc, width)
        gate_rows = lax.all_to_all(send_gate, 'ep', 1, 1, tiled=True).reshape(rows_loc)
        g_rows = (dy_rows.astype(F32) * gate_rows[:, None]).astype(BF16)

        part = down_grad(1 - z, h_gate, h_up, g_rows, fs_n)
        recv_down = exchange(part)
        dh_gate, dh_up = hidden_grads(z, g_rows, w_down, other_w_down, h_gate, h_up)
        part, = weight_grad_rhs(1 - z, x_rows, dh_gate, fs_n)
        recv_gate = exchange(part)
        step = width // fs_n // 16
        cuts = (0, 11 * step + step // 3, 15 * step, 15 * step + step // 3, 16 * step)
        piece = weight_grad_rhs(1 - z, x_rows, dh_up, fs_n, cuts)
        half = piece[2].shape[1] // 2
        direct, around = detour(piece[2][:, :half])
        plain = exchange(piece[2][:, half:])
        recv_up = [exchange(piece[0]), exchange(piece[1]), exchange(piece[3])]

        dx_rows = row_grads(z, dh_gate, dh_up, w_gate, other_w_gate, w_up, other_w_up)
        dgate_rows = jnp.einsum('rd,rd->r', dy_rows, y_rows, preferred_element_type=F32)
        back_dx = lax.all_to_all(dx_rows.reshape(e_loc, ep_n, slot_cap, width), 'ep', 1, 1, tiled=True).reshape(slots_n, width)
        back_gate = lax.all_to_all(dgate_rows.reshape(e_loc, ep_n, slot_cap), 'ep', 1, 1, tiled=True).reshape(slots_n)
        picked = jnp.take(back_dx, send_row, axis=0, mode='fill', fill_value=0).reshape(tok_n, top_n, width)
        grad_x = jnp.sum(picked.astype(F32), axis=1).astype(BF16)
        grad_gates = jnp.take(back_gate, send_row, mode='fill', fill_value=0).reshape(tok_n, top_n)

        grad_w_down = down_grad(z, h_gate, h_up, g_rows, fs_n, recv_down)
        grad_w_gate, = weight_grad_rhs(z, x_rows, dh_gate, fs_n, recv=recv_gate)
        grad_w_up, = weight_grad_rhs(z, x_rows, dh_up, fs_n, recv=recv_up[0])
        tail = grad_w_up[cuts[3]:]
        grad_w_up = add_piece(grad_w_up, jnp.concatenate([direct + around, plain], axis=1), cuts[2])
        grad_w_up = add_piece(grad_w_up, recv_up[1], cuts[1])
        grad_w_up = add_last(grad_w_up, tail, recv_up[-1])
        return grad_x, grad_gates, grad_w_gate[None], grad_w_down[None], grad_w_up[None]

    return jax.shard_map(local_backward, mesh=mesh, in_specs=(tok_spec, tok_spec, tok_spec, tok_spec, row_spec, row_spec, row_spec, row_spec, row_spec, row_spec, row_spec), out_specs=(tok_spec, tok_spec, row_spec, row_spec, row_spec), check_vma=False)
```

```python
import jax
import jax.numpy as jnp
from jax import lax
from jax.experimental import pallas as pl
from jax.experimental.pallas import tpu as pltpu
from jax.sharding import PartitionSpec as P


F32 = jnp.float32
BF16 = jnp.bfloat16
VMEM_LIMIT = 58 * 1024 * 1024


def params(*kinds):
    return pltpu.CompilerParams(dimension_semantics=kinds, vmem_limit_bytes=VMEM_LIMIT)


def cost(flops, bytes_accessed):
    return pl.CostEstimate(flops=flops, bytes_accessed=bytes_accessed, transcendentals=0)


def hidden_grads(z, g_rows, w_own, w_other, h_gate, h_up, row_tile=1280, col_tile=768):
    rows, width = g_rows.shape
    half = w_own.shape[0]
    tiles = half // col_tile
    row_steps = rows // row_tile

    def col(z_ref, h, j):
        return jnp.where(h == 0, z_ref[0], 1 - z_ref[0]) * tiles + j

    def kernel(z_ref, g_ref, own_ref, other_ref, h1_ref, h3_ref, d1_ref, d3_ref):
        h, i = pl.program_id(0), pl.program_id(2)
        g = g_ref[pl.ds(pl.multiple_of(i * row_tile, row_tile), row_tile), :]
        w = jnp.where(h == 0, own_ref[...], other_ref[...])
        d_act = lax.dot_general(g, w, (((1,), (1,)), ((), ())), preferred_element_type=F32)
        h1 = h1_ref[...].astype(F32)
        h3 = h3_ref[...].astype(F32)
        sig = jax.nn.sigmoid(h1)
        silu = h1 * sig
        d1_ref[...] = (d_act * h3 * sig * (1.0 + h1 * (1.0 - sig))).astype(BF16)
        d3_ref[...] = (d_act * silu).astype(BF16)

    tile = pl.BlockSpec((row_tile, col_tile), lambda h, j, i, z_ref: (i, col(z_ref, h, j)))
    return pl.pallas_call(
        kernel,
        grid_spec=pltpu.PrefetchScalarGridSpec(
            num_scalar_prefetch=1,
            grid=(2, tiles, row_steps),
            in_specs=[
                pl.BlockSpec((rows, width), lambda h, j, i, z_ref: (0, 0)),
                pl.BlockSpec((col_tile, width), lambda h, j, i, z_ref: (jnp.where(h == 0, j, tiles - 1), 0)),
                pl.BlockSpec((col_tile, width), lambda h, j, i, z_ref: (jnp.where(h == 0, 0, j), 0)),
                tile, tile,
            ],
            out_specs=[tile] * 2,
        ),
        out_shape=[jax.ShapeDtypeStruct(h_gate.shape, BF16)] * 2,
        compiler_params=params('arbitrary', 'arbitrary', 'arbitrary'),
        cost_estimate=cost(2 * rows * width * 2 * half, 8 * rows * 2 * half),
    )(z, g_rows, w_own, w_other, h_gate, h_up)


def down_grad(which, h_gate, h_up, g_rows, halves, recv=None, row_tile=1280, col_tile=512):
    rows, cols = h_gate.shape
    width = g_rows.shape[1]
    tiles = cols // halves // col_tile
    steps = rows // row_tile
    extra = [] if recv is None else [recv]

    def kernel(s_ref, h1_ref, h3_ref, g_ref, *refs):
        o_ref = refs[-1]
        i = pl.program_id(1)
        h1 = h1_ref[...].astype(F32)
        act = (h1 * jax.nn.sigmoid(h1) * h3_ref[...].astype(F32)).astype(BF16)
        g = g_ref[pl.ds(pl.multiple_of(i * row_tile, row_tile), row_tile), :]
        term = lax.dot_general(act, g, (((0,), (0,)), ((), ())), preferred_element_type=F32)

        @pl.when(i == 0)
        def _():
            o_ref[...] = term

        @pl.when(i > 0)
        def _():
            o_ref[...] += term

        if extra:
            @pl.when(i == steps - 1)
            def _():
                o_ref[...] += refs[0][...]

    out_tile = pl.BlockSpec((col_tile, width), lambda j, i, s_ref: (j, 0))
    tile = pl.BlockSpec((row_tile, col_tile), lambda j, i, s_ref: (i, s_ref[0] * tiles + j))
    return pl.pallas_call(
        kernel,
        grid_spec=pltpu.PrefetchScalarGridSpec(
            num_scalar_prefetch=1,
            grid=(tiles, steps),
            in_specs=[tile, tile, pl.BlockSpec((rows, width), lambda j, i, s_ref: (0, 0))] + [out_tile] * len(extra),
            out_specs=out_tile,
        ),
        out_shape=jax.ShapeDtypeStruct((tiles * col_tile, width), F32),
        compiler_params=params('arbitrary', 'arbitrary'),
        cost_estimate=cost(2 * rows * width * tiles * col_tile, 4 * rows * cols),
    )(which, h_gate, h_up, g_rows, *extra)


def weight_grad_rhs(which, x_rows, wide, halves, cuts=(), recv=None, col_tile=1024):
    rows, cols = wide.shape
    part = x_rows.shape[1] // halves
    cuts = cuts or (0, part)
    spans = list(zip(cuts, cuts[1:]))
    extra = [] if recv is None else [recv]

    def kernel(s_ref, l_ref, r_ref, *refs):
        o_refs = refs[len(extra):]
        total = lax.dot_general(l_ref[...], r_ref[...], (((0,), (0,)), ((), ())), preferred_element_type=F32)
        for o_ref, (lo, hi) in zip(o_refs, spans):
            o_ref[...] = total[lo:hi]
        if extra:
            o_refs[0][:recv.shape[0], :] += refs[0][...]

    return pl.pallas_call(
        kernel,
        grid_spec=pltpu.PrefetchScalarGridSpec(
            num_scalar_prefetch=1,
            grid=(cols // col_tile,),
            in_specs=[
                pl.BlockSpec((rows, part), lambda j, s_ref: (0, s_ref[0])),
                pl.BlockSpec((rows, col_tile), lambda j, s_ref: (0, j)),
            ] + [pl.BlockSpec((v.shape[0], col_tile), lambda j, s_ref: (0, j)) for v in extra],
            out_specs=[pl.BlockSpec((hi - lo, col_tile), lambda j, s_ref: (0, j)) for lo, hi in spans],
        ),
        out_shape=[jax.ShapeDtypeStruct((hi - lo, cols), F32) for lo, hi in spans],
        compiler_params=params('arbitrary'),
        cost_estimate=cost(2 * rows * part * cols, 2 * rows * cols + 4 * part * cols),
    )(which, x_rows, wide, *extra)


def row_grads(z, dh_gate, dh_up, gate_own, gate_other, up_own, up_other, row_tile=1280):
    rows, cols = dh_gate.shape
    part = gate_own.shape[0]

    def kernel(z_ref, d1_ref, d3_ref, g0_ref, g1_ref, u0_ref, u1_ref, o_ref):
        h = pl.program_id(0)
        dims = (((1,), (1,)), ((), ()))

        def emit(w1_ref, w3_ref):
            acc = lax.dot_general(d1_ref[...], w1_ref[...], dims, preferred_element_type=F32)
            acc += lax.dot_general(d3_ref[...], w3_ref[...], dims, preferred_element_type=F32)
            o_ref[...] = acc.astype(BF16)

        pl.when(h == 0)(lambda: emit(g0_ref, u0_ref))
        pl.when(h == 1)(lambda: emit(g1_ref, u1_ref))

    tile = pl.BlockSpec((row_tile, cols), lambda h, i, z_ref: (i, 0))
    full = pl.BlockSpec((part, cols), lambda h, i, z_ref: (0, 0), pipeline_mode=pl.Buffered(1))
    return pl.pallas_call(
        kernel,
        grid_spec=pltpu.PrefetchScalarGridSpec(
            num_scalar_prefetch=1,
            grid=(2, rows // row_tile),
            in_specs=[tile, tile, full, full, full, full],
            out_specs=pl.BlockSpec((row_tile, part), lambda h, i, z_ref: (i, jnp.where(h == 0, z_ref[0], 1 - z_ref[0]))),
        ),
        out_shape=jax.ShapeDtypeStruct((rows, 2 * part), BF16),
        compiler_params=params('arbitrary', 'arbitrary'),
        cost_estimate=cost(8 * rows * cols * part, 8 * rows * cols),
    )(z, dh_gate, dh_up, gate_own, gate_other, up_own, up_other)


def add_piece(own, recv, first):
    rows, width = recv.shape

    def kernel(own_ref, recv_ref, o_ref, here, there, sem):
        place = pl.ds(first, rows)
        ins = (pltpu.make_async_copy(own_ref.at[place], here, sem.at[0]), pltpu.make_async_copy(recv_ref, there, sem.at[1]))
        for copy in ins:
            copy.start()
        for copy in ins:
            copy.wait()
        here[...] += there[...]
        out = pltpu.make_async_copy(here, o_ref.at[place], sem.at[2])
        out.start()
        out.wait()

    return pl.pallas_call(
        kernel,
        in_specs=[pl.BlockSpec(memory_space=pl.ANY)] * 2,
        out_specs=pl.BlockSpec(memory_space=pl.ANY),
        out_shape=jax.ShapeDtypeStruct(own.shape, own.dtype),
        scratch_shapes=[pltpu.VMEM((rows, width), F32)] * 2 + [pltpu.SemaphoreType.DMA((3,))],
        input_output_aliases={0: 0},
        compiler_params=params(),
        cost_estimate=cost(rows * width, 12 * rows * width),
    )(own, recv)


def add_last(own, tail, recv):
    rows, width = recv.shape
    first = own.shape[0] - rows

    def kernel(own_ref, tail_ref, recv_ref, o_ref, total, sem):
        total[...] = tail_ref[...] + recv_ref[...]
        out = pltpu.make_async_copy(total, o_ref.at[pl.ds(first, rows)], sem)
        out.start()
        out.wait()

    vmem = pl.BlockSpec(memory_space=pltpu.VMEM)
    return pl.pallas_call(
        kernel,
        in_specs=[pl.BlockSpec(memory_space=pl.ANY), vmem, vmem],
        out_specs=pl.BlockSpec(memory_space=pl.ANY),
        out_shape=jax.ShapeDtypeStruct(own.shape, own.dtype),
        scratch_shapes=[pltpu.VMEM((rows, width), F32), pltpu.SemaphoreType.DMA],
        input_output_aliases={0: 0},
        compiler_params=pltpu.CompilerParams(vmem_limit_bytes=4 * 1024 * 1024),
        cost_estimate=cost(rows * width, 12 * rows * width),
    )(own, pltpu.with_memory_space_constraint(tail, pltpu.VMEM), pltpu.with_memory_space_constraint(recv, pltpu.VMEM))


def solution(mesh):
    ep_n = mesh.shape['ep']
    fs_n = mesh.shape['fsdp']
    tok_spec = P(('fsdp', 'ep'), None)
    row_spec = P('ep', 'fsdp', None)
    swap = [(i, fs_n - 1 - i) for i in range(fs_n)]

    def exchange(value):
        return lax.ppermute(value, 'fsdp', swap)

    near = 2
    far = range(1, ep_n // near)

    def send(value, moves):
        return lax.ppermute(value, ('fsdp', 'ep'), [(a * ep_n + b, c * ep_n + d) for (a, b), (c, d) in moves])

    def detour(value):
        cols = value.shape[1] // len(far)
        grid = [(f, c) for f in range(fs_n) for c in range(near)]
        rest = [((f, e), (fs_n - 1 - f, e)) for f in range(fs_n) for e in range(near, ep_n)]
        out = [send(value[:, (k - 1) * cols:k * cols], [((f, c), (f, near * k + c)) for f, c in grid]) for k in far]
        crossed = send(sum(out[1:], out[0]), rest)
        direct = send(value, rest)
        back = [send(crossed, [((f, near * k + c), (f, c)) for f, c in grid]) for k in far]
        return direct, jnp.concatenate(back, axis=1)

    def local_backward(grad_out, expert_idx, slot_pos, gates, x_disp, h_gate, h_up, y_disp, w_gate, w_down, w_up):
        tok_n, top_n = expert_idx.shape
        e_loc, rows_loc, width = x_disp.shape
        slot_cap = rows_loc // ep_n
        slots_n = e_loc * ep_n * slot_cap
        choices = tok_n * top_n
        x_rows, y_rows, h_gate, h_up, w_gate, w_down, w_up = (v[0] for v in (x_disp, y_disp, h_gate, h_up, w_gate, w_down, w_up))

        z = lax.axis_index('fsdp').reshape(1).astype(jnp.int32)
        other_w_down = exchange(w_down)
        other_w_gate = exchange(w_gate)
        other_w_up = exchange(w_up)

        send_row = jnp.where(slot_pos >= 0, ((expert_idx % e_loc) * ep_n + expert_idx // e_loc) * slot_cap + slot_pos, slots_n).reshape(-1)
        src_choice = jnp.full((slots_n,), choices, jnp.int32).at[send_row].set(jnp.arange(choices, dtype=jnp.int32), mode='drop')
        send_dy = jnp.take(grad_out, src_choice // top_n, axis=0, mode='clip').reshape(e_loc, ep_n, slot_cap, width)
        send_gate = jnp.take(gates.reshape(-1), src_choice, mode='fill', fill_value=0).reshape(e_loc, ep_n, slot_cap)
        dy_rows = lax.all_to_all(send_dy, 'ep', 1, 1, tiled=True).reshape(rows_loc, width)
        gate_rows = lax.all_to_all(send_gate, 'ep', 1, 1, tiled=True).reshape(rows_loc)
        g_rows = (dy_rows.astype(F32) * gate_rows[:, None]).astype(BF16)

        part = down_grad(1 - z, h_gate, h_up, g_rows, fs_n)
        recv_down = exchange(part)
        dh_gate, dh_up = hidden_grads(z, g_rows, w_down, other_w_down, h_gate, h_up)
        part, = weight_grad_rhs(1 - z, x_rows, dh_gate, fs_n)
        recv_gate = exchange(part)
        step = width // fs_n // 16
        cuts = (0, 11 * step + 2 * step // 3, 15 * step, 15 * step + step // 3, 16 * step)
        piece = weight_grad_rhs(1 - z, x_rows, dh_up, fs_n, cuts)
        half = piece[2].shape[1] // 2
        direct, around = detour(piece[2][:, :half])
        plain = exchange(piece[2][:, half:])
        recv_up = [exchange(piece[0]), exchange(piece[1]), exchange(piece[3])]

        dx_rows = row_grads(z, dh_gate, dh_up, w_gate, other_w_gate, w_up, other_w_up)
        dgate_rows = jnp.einsum('rd,rd->r', dy_rows, y_rows, preferred_element_type=F32)
        back_dx = lax.all_to_all(dx_rows.reshape(e_loc, ep_n, slot_cap, width), 'ep', 1, 1, tiled=True).reshape(slots_n, width)
        back_gate = lax.all_to_all(dgate_rows.reshape(e_loc, ep_n, slot_cap), 'ep', 1, 1, tiled=True).reshape(slots_n)
        picked = jnp.take(back_dx, send_row, axis=0, mode='fill', fill_value=0).reshape(tok_n, top_n, width)
        grad_x = jnp.sum(picked.astype(F32), axis=1).astype(BF16)
        grad_gates = jnp.take(back_gate, send_row, mode='fill', fill_value=0).reshape(tok_n, top_n)

        grad_w_down = down_grad(z, h_gate, h_up, g_rows, fs_n, recv_down)
        grad_w_gate, = weight_grad_rhs(z, x_rows, dh_gate, fs_n, recv=recv_gate)
        grad_w_up, = weight_grad_rhs(z, x_rows, dh_up, fs_n, recv=recv_up[0])
        tail = grad_w_up[cuts[3]:]
        grad_w_up = add_piece(grad_w_up, jnp.concatenate([direct + around, plain], axis=1), cuts[2])
        grad_w_up = add_piece(grad_w_up, recv_up[1], cuts[1])
        grad_w_up = add_last(grad_w_up, tail, recv_up[-1])
        return grad_x, grad_gates, grad_w_gate[None], grad_w_down[None], grad_w_up[None]

    return jax.shard_map(local_backward, mesh=mesh, in_specs=(tok_spec, tok_spec, tok_spec, tok_spec, row_spec, row_spec, row_spec, row_spec, row_spec, row_spec, row_spec), out_specs=(tok_spec, tok_spec, row_spec, row_spec, row_spec), check_vma=False)
```
